32 devices in a mesh: dp: 4 (over y, core), mp: 8 (over z, x).
Axes of the slice: x: 2, y: 2, z: 4, core: 2. Of those that a mesh axis runs over, the one named last changes fastest.
Arguments:
- hidden: bfloat16 [8192, 2048], P(('dp', 'mp')), may hold values from -6 to 6
- lengths: int32 [4], P('dp'), may hold values from 1024 to 2048, as said below
- pre_gain: float32 [2, 2048], replicated, may hold values from 0.5 to 1.5
- w_inner: bfloat16 [2, 2048, 2, 4096], P(None, None, None, 'mp'), may hold values from -0.125 to 0.125
- w_step: bfloat16 [2, 2048, 64], P(None, None, 'mp'), may hold values from -0.125 to 0.125
- w_shared: bfloat16 [2, 2048, 256], replicated, may hold values from -0.125 to 0.125
- conv_inner: float32 [2, 4, 4096], P(None, None, 'mp'), may hold values from -3 to 3
- conv_inner_bias: float32 [2, 4096], P(None, 'mp'), may hold values from -2 to 2
- conv_shared: float32 [2, 4, 256], replicated, may hold values from -3 to 3
- conv_shared_bias: float32 [2, 256], replicated, may hold values from -2 to 2
- step_bias: float32 [2, 64], P(None, 'mp'), may hold values from -5 to -2.5
- decay_log: float32 [2, 64], P(None, 'mp'), may hold values from -2.5 to 0.5
- skip_gain: float32 [2, 64], P(None, 'mp'), may hold values from 0.5 to 1.5
- norm_gain: float32 [2, 4096], P(None, 'mp'), may hold values from 0.5 to 1.5
- w_out: bfloat16 [2, 4096, 2048], P(None, 'mp'), may hold values from -0.09375 to 0.09375
- out_grad: bfloat16 [8192, 2048], P(('dp', 'mp')), may hold values from -6 to 6
Outputs:
- first_out: float32 [8192, 2048], P(('dp', 'mp'))
- second_out: float32 [8192, 2048], P(('dp', 'mp'))
- hidden_grad: float32 [8192, 2048], P(('dp', 'mp'))
- pre_gain_grad: float32 [2, 2048], replicated
- w_inner_grad: float32 [2, 2048, 2, 4096], P(None, None, None, 'mp')
- w_step_grad: float32 [2, 2048, 64], P(None, None, 'mp')
- w_shared_grad: float32 [2, 2048, 256], replicated
- conv_inner_grad: float32 [2, 4, 4096], P(None, None, 'mp')
- conv_inner_bias_grad: float32 [2, 4096], P(None, 'mp')
- conv_shared_grad: float32 [2, 4, 256], replicated
- conv_shared_bias_grad: float32 [2, 256], replicated
- step_bias_grad: float32 [2, 64], P(None, 'mp')
- decay_log_grad: float32 [2, 64], P(None, 'mp')
- skip_gain_grad: float32 [2, 64], P(None, 'mp')
- norm_gain_grad: float32 [2, 4096], P(None, 'mp')
- w_out_grad: float32 [2, 4096, 2048], P(None, 'mp')
The draws below stay inside these ranges and needn't reach their ends.
Inputs may be any that keep to these rules, and one draw needn't show every extreme that they name: lengths[s] is the number of live tokens at the start of slot s; at least one slot is full, holding 2048 tokens.
All inputs are finite; a program needn't handle non-finite values.
Results may differ from the reference program's by a relative error of at most 0.03.
Values may be sent and summed in bfloat16 or wider, within the bound.
A program may use at most 512 MiB of HBM per device.

```python
import jax
import jax.numpy as jnp
from jax import lax

D = 2048
HEADS = 64
HEAD_DIM = 64
STATE = 128
CONV = 4
BLOCK = 256
BUCKET = 2048
LAYERS = 2
INNER = 4096
TOKENS = 8192
SEQS = 4


def draw_lengths(key, part):
    first, second = jax.random.split(jax.random.fold_in(key, 11))
    drawn = jax.random.randint(first, (SEQS,), BUCKET // 2, BUCKET + 1)
    chosen = jax.random.randint(second, (), 0, SEQS)
    places = jnp.arange(SEQS)
    return jnp.where(places == chosen, BUCKET, drawn).astype(jnp.int32)


def shard_levels(own_key, shape, cuts, smallest, largest):
    gain = 1.0
    for axis_at, blocks in cuts:
        heights = jax.random.uniform(jax.random.fold_in(jax.random.fold_in(own_key, 6), axis_at), (blocks,), jnp.float32, smallest / len(cuts), largest / len(cuts))
        gain = gain * jnp.repeat(jnp.exp(heights), shape[axis_at] // blocks).reshape((-1,) + (1,) * (len(shape) - 1 - axis_at))
    return gain


def bell_draw(key, extent, scale, bound, cuts=(), kind=jnp.bfloat16):
    result = scale * jax.random.normal(key, extent, jnp.float32)
    if cuts:
        result = result * shard_levels(key, extent, cuts, -0.22, 0.18)
    return jnp.clip(result, -bound, bound).astype(kind)


def setup_inputs(seed: int = 0) -> dict:
    key_list = jax.random.split(jax.random.key(seed), 17)
    return {
        "hidden": bell_draw(key_list[0], (TOKENS, D), 1.0, 6.0, ((0, 32),)),
        "lengths": draw_lengths(jax.random.fold_in(key_list[16], 71), 0),
        "pre_gain": jnp.clip(1.0 + 0.1 * jax.random.normal(key_list[2], (LAYERS, D), jnp.float32), 0.5, 1.5),
        "w_inner": bell_draw(key_list[3], (LAYERS, D, 2, INNER), D ** -0.5, 0.125, ((3, 8),)),
        "w_step": bell_draw(key_list[4], (LAYERS, D, HEADS), D ** -0.5, 0.125, ((2, 8),)),
        "w_shared": bell_draw(key_list[5], (LAYERS, D, 2 * STATE), D ** -0.5, 0.125),
        "conv_inner": bell_draw(key_list[6], (LAYERS, CONV, INNER), CONV ** -0.5, 3.0, ((2, 8),), jnp.float32),
        "conv_inner_bias": bell_draw(key_list[7], (LAYERS, INNER), 0.3, 2.0, ((1, 8),), jnp.float32),
        "conv_shared": bell_draw(key_list[8], (LAYERS, CONV, 2 * STATE), CONV ** -0.5, 3.0, (), jnp.float32),
        "conv_shared_bias": bell_draw(key_list[9], (LAYERS, 2 * STATE), 0.3, 2.0, (), jnp.float32),
        "step_bias": jnp.clip(-5.0 + 2.5 * jax.random.uniform(key_list[10], (LAYERS, HEADS), jnp.float32) ** shard_levels(key_list[10], (LAYERS, HEADS), ((1, 8),), -0.2, 0.2), -5.0, -2.5),
        "decay_log": jnp.clip(-2.5 + 3.0 * jax.random.uniform(key_list[11], (LAYERS, HEADS), jnp.float32) ** shard_levels(key_list[11], (LAYERS, HEADS), ((1, 8),), -0.2, 0.2), -2.5, 0.5),
        "skip_gain": jnp.clip(0.5 + 1.0 * jax.random.uniform(key_list[12], (LAYERS, HEADS), jnp.float32) ** shard_levels(key_list[12], (LAYERS, HEADS), ((1, 8),), -0.2, 0.2), 0.5, 1.5),
        "norm_gain": jnp.clip(1.0 + 0.1 * jax.random.normal(key_list[13], (LAYERS, INNER), jnp.float32), 0.5, 1.5),
        "w_out": bell_draw(key_list[14], (LAYERS, INNER, D), INNER ** -0.5, 0.09375, ((1, 8),)),
        "out_grad": bell_draw(key_list[15], (TOKENS, D), 1.0, 6.0, ((0, 32),)),
    }


EPSILON = 1e-05
HIGH = lax.Precision.HIGHEST

@jax.custom_vjp
def low(v):
    return lax.optimization_barrier(v.astype(jnp.bfloat16)).astype(jnp.float32)

@jax.custom_vjp
def low_back(v):
    return v

def low_keep(v):
    return (low(v), None)

def low_pass(kept, grad):
    return (grad,)

def back_keep(v):
    return (v, None)

def back_low(kept, grad):
    return (low(grad),)
low.defvjp(low_keep, low_pass)
low_back.defvjp(back_keep, back_low)

def causal_conv(values, weight, bias):
    rows, width = values.shape
    taps = weight.shape[0]
    slots = values.reshape(rows // BUCKET, BUCKET, width)
    padded = jnp.pad(slots, ((0, 0), (taps - 1, 0), (0, 0)))
    total = bias + jnp.zeros_like(slots)
    for lag in range(taps):
        total = total + weight[lag] * padded[:, taps - 1 - lag:taps - 1 - lag + BUCKET]
    return total.reshape(rows, width)

def slot_scan(values, delta, inputs_b, inputs_c, decay):
    length, heads, width = values.shape
    count = length // BLOCK
    states = inputs_b.shape[-1]
    values = values.reshape(count, BLOCK, heads, width)
    delta = delta.reshape(count, BLOCK, heads)
    inputs_b = inputs_b.reshape(count, BLOCK, states)
    inputs_c = inputs_c.reshape(count, BLOCK, states)
    logs = jnp.cumsum(delta * decay, axis=1)
    rows_index = lax.broadcasted_iota(jnp.int32, (BLOCK, BLOCK), 0)
    cols_index = lax.broadcasted_iota(jnp.int32, (BLOCK, BLOCK), 1)
    lower = (rows_index >= cols_index)[None, :, :, None]
    gaps = jnp.where(lower, logs[:, :, None, :] - logs[:, None, :, :], 0.0)
    within = jnp.where(lower, jnp.exp(gaps), 0.0)
    scores = jnp.einsum('cin,cjn->cij', inputs_c, inputs_b, precision=HIGH)
    weighted = values * delta[..., None]
    direct = jnp.einsum('cij,cijh,cjhp->cihp', scores, within, weighted, precision=HIGH)
    tails = jnp.exp(logs[:, -1:, :] - logs)
    local_states = jnp.einsum('cjn,cjh,cjhp->chpn', inputs_b, tails, weighted, precision=HIGH)
    totals = jnp.exp(logs[:, -1, :])

    def advance(carry, pieces):
        return (carry * pieces[1][:, None, None] + pieces[0], carry)
    begin = jnp.zeros((heads, width, states), jnp.float32)
    _, entering = lax.scan(advance, begin, (local_states, totals))
    carried = jnp.einsum('cin,chpn,cih->cihp', inputs_c, entering, jnp.exp(logs), precision=HIGH)
    return (direct + carried).reshape(length, heads, width)

def mixer(pad_mask, gate_inner, step_raw, shared_raw, conv_inner, conv_inner_bias, conv_shared, conv_shared_bias, step_bias, decay_log, skip_gain):
    rows = gate_inner.shape[0]
    heads = step_raw.shape[1]
    states = shared_raw.shape[1] // 2
    slots = rows // BUCKET
    channels = jax.nn.silu(causal_conv(gate_inner[:, 1], conv_inner, conv_inner_bias)) * pad_mask[:, None]
    shared = jax.nn.silu(causal_conv(shared_raw, conv_shared, conv_shared_bias)) * pad_mask[:, None]
    delta = jax.nn.softplus(step_raw + step_bias)
    decay = -jnp.exp(decay_log)
    values = channels.reshape(slots, BUCKET, heads, HEAD_DIM)

    def one_slot(pieces):
        return slot_scan(pieces[0], pieces[1], pieces[2], pieces[3], decay)
    mixed = lax.map(jax.checkpoint(one_slot), (values, delta.reshape(slots, BUCKET, heads), shared[:, :states].reshape(slots, BUCKET, states), shared[:, states:].reshape(slots, BUCKET, states)))
    mixed = mixed + skip_gain[:, None] * values
    return mixed.reshape(rows, heads * HEAD_DIM) * jax.nn.silu(gate_inner[:, 0])

def block(state, pad_mask, pre_gain, w_inner, w_step, w_shared, conv_inner, conv_inner_bias, conv_shared, conv_shared_bias, step_bias, decay_log, skip_gain, norm_gain, w_out):
    base = state * lax.rsqrt(lax.optimization_barrier(jnp.mean(state * state, axis=-1, keepdims=True)) + EPSILON)
    normed = low(base * pre_gain)
    gate_inner = low_back(jnp.einsum('td,dkc->tkc', normed, w_inner, precision=HIGH))
    step_raw = low_back(jnp.dot(normed, w_step, precision=HIGH))
    shared_raw = low_back(jnp.dot(normed, w_shared, precision=HIGH))
    gated = mixer(pad_mask, gate_inner, step_raw, shared_raw, conv_inner, conv_inner_bias, conv_shared, conv_shared_bias, step_bias, decay_log, skip_gain)
    unit = gated * lax.rsqrt(lax.optimization_barrier(jnp.mean(gated * gated, axis=-1, keepdims=True)) + EPSILON)
    scaled = low(unit * norm_gain)
    return state + low_back(jnp.dot(scaled, w_out, precision=HIGH))

def reference(hidden, lengths, pre_gain, w_inner, w_step, w_shared, conv_inner, conv_inner_bias, conv_shared, conv_shared_bias, step_bias, decay_log, skip_gain, norm_gain, w_out, out_grad):
    places = lax.broadcasted_iota(jnp.int32, (lengths.shape[0], BUCKET), 1)
    pad_mask = (places < lengths[:, None]).astype(jnp.float32).reshape(-1)
    weights = (pre_gain.astype(jnp.float32), w_inner.astype(jnp.float32), w_step.astype(jnp.float32), w_shared.astype(jnp.float32), conv_inner.astype(jnp.float32), conv_inner_bias.astype(jnp.float32), conv_shared.astype(jnp.float32), conv_shared_bias.astype(jnp.float32), step_bias.astype(jnp.float32), decay_log.astype(jnp.float32), skip_gain.astype(jnp.float32), norm_gain.astype(jnp.float32), w_out.astype(jnp.float32))

    def forward(state, *params):
        first = block(state, pad_mask, *[item[0] for item in params])
        second = block(first, pad_mask, *[item[1] for item in params])
        return (first, second)
    (first_out, second_out), pull = jax.vjp(forward, hidden.astype(jnp.float32), *weights)
    grads = pull((jnp.zeros_like(first_out), out_grad.astype(jnp.float32)))
    return (first_out, second_out, grads[0], grads[1], grads[2], grads[3], grads[4], grads[5], grads[6], grads[7], grads[8], grads[9], grads[10], grads[11], grads[12], grads[13])
```

```python
import itertools
import math

import jax
import jax.numpy as jnp
from jax import lax
from jax.experimental import pallas as pl
from jax.experimental.pallas import tpu as pltpu
from jax.sharding import PartitionSpec as P

HEAD_DIM = 64
STATE = 128
BUCKET = 2048
LAYERS = 2
CHUNK = 128
SMALL = 3 * STATE
EPSILON = 1e-05
LOG2E = math.log2(math.e)
VMEM_LIMIT = 56 << 20
AXES = ("dp", "mp")
BF = jnp.bfloat16
F32 = jnp.float32


def mm(a, b, dims=((1,), (0,))):
    return lax.dot_general(a, b, (dims, ((), ())), preferred_element_type=F32)


def mm_exact(a, b, dims=((1,), (0,))):
    return lax.dot_general(
        a, b, (dims, ((), ())), preferred_element_type=F32, precision=lax.Precision.HIGHEST
    )


def mm_split(a, ones):
    high = a.astype(BF)
    return mm(high, ones) + mm((a - high.astype(F32)).astype(BF), ones)


def sigmoid(v):
    return 0.5 * jnp.tanh(0.5 * v) + 0.5


def iota(shape, axis):
    return lax.broadcasted_iota(jnp.int32, shape, axis)


def softplus(v):
    return jnp.maximum(v, 0.0) + jnp.log1p(jnp.exp(-jnp.abs(v)))


def step_terms(step_raw, head_ref, lower):
    shifted = step_raw + head_ref[0:1, :]
    delta = softplus(shifted)
    logs = mm_exact(lower, delta * (head_ref[1:2, :] * LOG2E))
    return shifted, delta, logs, logs.T


def column(values, head):
    return jnp.broadcast_to(values[:, head : head + 1], (values.shape[0], 128))


def forward_kernel(cross, v_ref, len_ref, *refs):
    if cross:
        proj_ref, chan_ref, shr_ref, head_ref, dsc_ref, *refs = refs
    else:
        proj_ref, chan_ref, shr_ref, head_ref, *refs = refs
    h_ref, mixed_ref, st_ref, sums_ref, raw_buf, shr_buf, state = refs
    width = h_ref.shape[1]
    length = CHUNK
    chunk = pl.program_id(1)

    @pl.when(chunk == 0)
    def _():
        raw_buf[0:8, :] = jnp.zeros((8, width), F32)
        shr_buf[0:8, :] = jnp.zeros((8, 2 * STATE), F32)
        state[...] = jnp.zeros_like(state)

    mask = (chunk * length + iota((length, 128), 0) < len_ref[pl.program_id(0)]).astype(F32)
    row, col = iota((length, length), 0), iota((length, length), 1)
    lower = row >= col
    low_half = iota((length, 128), 1) < HEAD_DIM

    shr_buf[8 : 8 + length, :] = proj_ref[:, 2 * width : 2 * width + 2 * STATE].astype(F32)
    parts = []
    for part in range(2):
        lanes = slice(part * STATE, (part + 1) * STATE)
        pre = shr_ref[4:5, lanes] + shr_ref[0:1, lanes] * shr_buf[8 : 8 + length, lanes]
        for lag in range(1, 4):
            pre = pre + shr_ref[lag : lag + 1, lanes] * shr_buf[8 - lag : 8 - lag + length, lanes]
        parts.append((pre * sigmoid(pre) * mask).astype(BF))
    b_low, c_low = parts
    shr_buf[0:8, :] = shr_buf[length : length + 8, :]
    scores = mm(c_low, b_low, ((1,), (1,)))

    step_raw = proj_ref[:, 2 * width + 2 * STATE : 2 * width + 3 * STATE].astype(F32)
    _, delta, logs, logs_t = step_terms(step_raw, head_ref, lower.astype(F32))

    raw_buf[8 : 8 + length, :] = proj_ref[:, width : 2 * width].astype(F32)
    state_low = state[...].astype(BF)
    st_ref[0] = state_low
    ones = jnp.ones((8, 128), BF)
    square = jnp.zeros((8, length), F32)
    crossing = jnp.zeros((8, length), F32)
    for pair in range(width // 128):
        lanes = slice(pair * 128, pair * 128 + 128)
        pre = chan_ref[4:5, lanes] + chan_ref[0:1, lanes] * raw_buf[8 : 8 + length, lanes]
        for lag in range(1, 4):
            pre = pre + chan_ref[lag : lag + 1, lanes] * raw_buf[8 - lag : 8 - lag + length, lanes]
        x = pre * sigmoid(pre) * mask
        cols = (column(logs, 2 * pair), column(logs, 2 * pair + 1))
        logs_pair = jnp.where(low_half, cols[0], cols[1])
        u = x * jnp.where(low_half, column(delta, 2 * pair), column(delta, 2 * pair + 1))
        weights = []
        for half in range(2):
            head = 2 * pair + half
            gap = jnp.where(lower, cols[half] - logs_t[head : head + 1, :], -1e30)
            weights.append((scores * jnp.exp2(gap)).astype(BF))
        u_low = u.astype(BF)
        zero = jnp.zeros_like(u_low)
        direct = mm(
            jnp.concatenate(weights, axis=1),
            jnp.concatenate([jnp.where(low_half, u_low, zero), jnp.where(low_half, zero, u_low)], axis=0),
        )
        carried = mm(c_low, state_low[:, lanes])
        mixed = direct + jnp.exp2(logs_pair) * carried + chan_ref[6:7, lanes] * x
        mixed_ref[:, lanes] = mixed.astype(BF)
        total = logs_pair[length - 1 : length, :]
        fresh = mm(b_low, (u * jnp.exp2(total - logs_pair)).astype(BF), ((0,), (0,)))
        state[:, lanes] = state[:, lanes] * jnp.exp2(total) + fresh
        gate = proj_ref[:, lanes].astype(F32)
        gated = mixed * (gate * sigmoid(gate))
        scaled = gated * chan_ref[5:6, lanes]
        h_ref[:, lanes] = scaled.astype(BF)
        square = square + mm(ones, (gated * gated).astype(BF), ((1,), (1,)))
        if cross:
            product = dsc_ref[:, lanes].astype(F32) * scaled
            high = product.astype(BF)
            rest = (product - high.astype(F32)).astype(BF)
            crossing = crossing + mm(ones, high, ((1,), (1,))) + mm(ones, rest, ((1,), (1,)))
    raw_buf[0:8, :] = raw_buf[length : length + 8, :]
    sums_ref[0] = jnp.where(iota((8, length), 0) == 0, square, crossing)


def backward_kernel(v_ref, len_ref, *refs):
    (proj_ref, tail_ref, mixed_ref, dsc_ref, st_ref, rat_ref, chan_ref, shr_ref, head_ref) = refs[:9]
    (low_ref, scaled_ref, g_chan_ref, g_shr_ref, g_head_ref) = refs[9:14]
    (raw_buf, shr_buf, dpre_buf, dshr_buf, d_state, u_all, ey_all) = refs[14:]
    width = mixed_ref.shape[1]
    pairs = width // 128
    length = CHUNK
    step = pl.program_id(1)
    chunk = pl.num_programs(1) - 1 - step

    @pl.when(step == 0)
    def _():
        dpre_buf[length : length + 8, :] = jnp.zeros((8, width), F32)
        dshr_buf[length : length + 8, :] = jnp.zeros((8, 2 * STATE), F32)
        d_state[...] = jnp.zeros_like(d_state)

    @pl.when((step == 0) & (pl.program_id(0) == 0))
    def _():
        g_chan_ref[...] = jnp.zeros_like(g_chan_ref)
        g_shr_ref[...] = jnp.zeros_like(g_shr_ref)
        g_head_ref[...] = jnp.zeros_like(g_head_ref)

    mask = (chunk * length + iota((length, 128), 0) < len_ref[pl.program_id(0)]).astype(F32)
    row, col = iota((length, length), 0), iota((length, length), 1)
    lower = row >= col
    lower_f = lower.astype(F32)
    upper_f = (row <= col).astype(F32)
    strict_f = (row > col).astype(F32)
    lane = iota((length, 128), 1)
    low_half = lane < HEAD_DIM
    inside = (chunk > 0).astype(F32)

    shr_buf[0:8, :] = tail_ref[8:16, 2 * width : 2 * width + 2 * STATE].astype(F32) * inside
    shr_buf[8 : 8 + length, :] = proj_ref[:, 2 * width : 2 * width + 2 * STATE].astype(F32)
    parts, slopes = [], []
    for part in range(2):
        lanes = slice(part * STATE, (part + 1) * STATE)
        pre = shr_ref[4:5, lanes] + shr_ref[0:1, lanes] * shr_buf[8 : 8 + length, lanes]
        for lag in range(1, 4):
            pre = pre + shr_ref[lag : lag + 1, lanes] * shr_buf[8 - lag : 8 - lag + length, lanes]
        s = sigmoid(pre)
        value = pre * s
        parts.append((value * mask).astype(BF))
        slopes.append(mask * (s + value * (1.0 - s)))
    b_low, c_low = parts
    scores = mm(c_low, b_low, ((1,), (1,)))

    step_raw = proj_ref[:, 2 * width + 2 * STATE : 2 * width + 3 * STATE].astype(F32)
    shifted, delta, logs, logs_t = step_terms(step_raw, head_ref, lower_f)
    scales = rat_ref[0].T
    ratio = jnp.broadcast_to(scales[:, 0:1], (length, 128))
    pull = jnp.broadcast_to(scales[:, 1:2], (length, 128))

    raw_buf[0:8, :] = tail_ref[8:16, width : 2 * width].astype(F32) * inside
    raw_buf[8 : 8 + length, :] = proj_ref[:, width : 2 * width].astype(F32)

    d_scores = jnp.zeros((length, length), F32)
    rows_sum = jnp.zeros((length, 128), F32)
    cols_sum = jnp.zeros((8, length), F32)
    before = jnp.zeros((length, 128), F32)
    after = jnp.zeros((length, 128), F32)
    d_delta = jnp.zeros((length, 128), F32)
    leaving = jnp.zeros((8, 128), F32)
    for pair in range(pairs):
        lanes = slice(pair * 128, pair * 128 + 128)
        heads = (iota((128, 128), 1) == 2 * pair + iota((128, 128), 0) // HEAD_DIM).astype(BF)
        gain = chan_ref[5:6, lanes]
        gate = proj_ref[:, lanes].astype(F32)
        mixed = mixed_ref[:, lanes].astype(F32)
        dsc = dsc_ref[:, lanes].astype(F32)
        s = sigmoid(gate)
        swish = gate * s
        gated = mixed * swish
        unit = gated * ratio
        g_chan_ref[5:6, lanes] += jnp.sum(dsc * unit, axis=0, keepdims=True)
        scaled_ref[:, lanes] = (unit * gain).astype(BF)
        d_gated = ratio * (dsc * gain) - gated * pull
        dy = d_gated * swish
        low_ref[:, lanes] = (d_gated * mixed * (s + swish * (1.0 - s))).astype(BF)
        pre = chan_ref[4:5, lanes] + chan_ref[0:1, lanes] * raw_buf[8 : 8 + length, lanes]
        for lag in range(1, 4):
            pre = pre + chan_ref[lag : lag + 1, lanes] * raw_buf[8 - lag : 8 - lag + length, lanes]
        s = sigmoid(pre)
        value = pre * s
        x = value * mask
        slope = mask * (s + value * (1.0 - s))
        g_chan_ref[6:7, lanes] += jnp.sum(dy * x, axis=0, keepdims=True)
        cols = (column(logs, 2 * pair), column(logs, 2 * pair + 1))
        logs_pair = jnp.where(low_half, cols[0], cols[1])
        delta_pair = jnp.where(low_half, column(delta, 2 * pair), column(delta, 2 * pair + 1))
        u = x * delta_pair
        u_low = u.astype(BF)
        dy_low = dy.astype(BF)
        zero = jnp.zeros_like(dy_low)
        dy_two = jnp.concatenate(
            [jnp.where(low_half, dy_low, zero), jnp.where(low_half, zero, dy_low)], axis=0
        )
        d_weights = mm(dy_two, u_low, ((1,), (1,)))
        weights = []
        for half in range(2):
            head = 2 * pair + half
            fade = jnp.exp2(jnp.where(lower, cols[half] - logs_t[head : head + 1, :], -1e30))
            weights.append((scores * fade).astype(BF))
            pulled = d_weights[half * length : (half + 1) * length, :] * fade
            d_scores = d_scores + pulled
            moved = pulled * scores
            rows_sum = jnp.where(lane == head, jnp.sum(moved, axis=1, keepdims=True), rows_sum)
            cols_sum = jnp.where(
                iota((8, length), 0) == head, jnp.sum(moved, axis=0, keepdims=True), cols_sum
            )
        d_u = mm(jnp.concatenate(weights, axis=0), dy_two, ((0,), (0,)))
        rise = jnp.exp2(logs_pair)
        total = logs_pair[length - 1 : length, :]
        fall = jnp.exp2(total - logs_pair)
        state_low = st_ref[0, :, lanes]
        d_next = d_state[:, lanes]
        d_next_low = d_next.astype(BF)
        e_dy = dy * rise
        e_low = e_dy.astype(BF)
        ey_all[:, lanes] = e_low
        u_all[:, lanes] = (u * fall).astype(BF)
        rows_sum = rows_sum + mm_split(e_dy * mm(c_low, state_low), heads)
        through = fall * mm(b_low, d_next_low)
        before = before + mm_split(u * through, heads)
        d_u = d_u + through
        d_delta = d_delta + mm_split(x * d_u, heads)
        whole = jnp.exp2(total)
        kept = jnp.sum(state_low.astype(F32) * d_next, axis=0, keepdims=True) * whole
        leaving = leaving + mm_split(jnp.broadcast_to(kept, (8, 128)), heads)
        d_state[:, lanes] = d_next * whole + mm(c_low, e_low, ((0,), (0,)))
        after = after + mm(e_low, state_low, ((1,), (1,)))
        shr_part = mm(u_all[:, lanes], d_next_low, ((1,), (1,)))
        if pair == 0:
            d_b = shr_part
        else:
            d_b = d_b + shr_part
        d_x = delta_pair * d_u + chan_ref[6:7, lanes] * dy
        d_pre = d_x * slope
        dpre_buf[0:length, lanes] = d_pre
        g_chan_ref[4:5, lanes] += jnp.sum(d_pre, axis=0, keepdims=True)
        d_raw = chan_ref[0:1, lanes] * d_pre
        g_chan_ref[0:1, lanes] += jnp.sum(d_pre * raw_buf[8 : 8 + length, lanes], axis=0, keepdims=True)
        for lag in range(1, 4):
            d_raw = d_raw + chan_ref[lag : lag + 1, lanes] * dpre_buf[lag : lag + length, lanes]
            g_chan_ref[lag : lag + 1, lanes] += jnp.sum(
                d_pre * raw_buf[8 - lag : 8 - lag + length, lanes], axis=0, keepdims=True
            )
        low_ref[:, width + pair * 128 : width + pair * 128 + 128] = d_raw.astype(BF)
    dpre_buf[length : length + 8, :] = dpre_buf[0:8, :]

    ds_low = d_scores.astype(BF)
    d_b = d_b + mm(ds_low, c_low, ((0,), (0,)))
    d_c = after + mm(ds_low, b_low)
    for part, value in enumerate((d_b, d_c)):
        lanes = slice(part * STATE, (part + 1) * STATE)
        d_pre = value * slopes[part]
        dshr_buf[0:length, lanes] = d_pre
        g_shr_ref[4:5, lanes] += jnp.sum(d_pre, axis=0, keepdims=True)
        d_raw = shr_ref[0:1, lanes] * d_pre
        g_shr_ref[0:1, lanes] += jnp.sum(d_pre * shr_buf[8 : 8 + length, lanes], axis=0, keepdims=True)
        for lag in range(1, 4):
            d_raw = d_raw + shr_ref[lag : lag + 1, lanes] * dshr_buf[lag : lag + length, lanes]
            g_shr_ref[lag : lag + 1, lanes] += jnp.sum(
                d_pre * shr_buf[8 - lag : 8 - lag + length, lanes], axis=0, keepdims=True
            )
        low_ref[:, 2 * width + part * STATE : 2 * width + (part + 1) * STATE] = d_raw.astype(BF)
    dshr_buf[length : length + 8, :] = dshr_buf[0:8, :]

    cols_all = jnp.concatenate([cols_sum, jnp.zeros((length - 8, length), F32)], axis=0)
    d_log = (
        mm_exact(upper_f, rows_sum)
        - mm_exact(upper_f, cols_all, ((1,), (1,)))
        + mm_exact(strict_f, before)
        + leaving[0:1, :]
    )
    d_delta = d_delta + head_ref[1:2, :] * d_log
    d_step = d_delta * sigmoid(shifted)
    low_ref[:, 2 * width + 2 * STATE : 2 * width + 3 * STATE] = d_step.astype(BF)
    g_head_ref[0:1, :] += jnp.sum(d_step, axis=0, keepdims=True)
    g_head_ref[1:2, :] += jnp.sum(delta * d_log, axis=0, keepdims=True)


def chunk_index(own_rows, count):
    per_block = own_rows // CHUNK

    def place(slot, chunk, v):
        return slot * count + ((chunk // per_block) ^ v) * per_block + chunk % per_block

    return place


def mixer_forward(v, lengths, own_rows, proj, chan, shr, head, dsc=None):
    rows = proj.shape[0]
    width = chan.shape[1]
    slots, count = rows // BUCKET, BUCKET // CHUNK
    place = chunk_index(own_rows, count)

    def tokens(slot, chunk, v_ref, len_ref):
        return (place(slot, chunk, v_ref[0]), 0)

    def blocks(slot, chunk, v_ref, len_ref):
        return (place(slot, chunk, v_ref[0]), 0, 0)

    def fixed(slot, chunk, v_ref, len_ref):
        return (0, 0)

    def in_order(slot, chunk, v_ref, len_ref):
        return (slot * count + chunk, 0, 0)

    in_specs = [
        pl.BlockSpec((CHUNK, proj.shape[1]), tokens),
        pl.BlockSpec((8, width), fixed),
        pl.BlockSpec((8, 2 * STATE), fixed),
        pl.BlockSpec((8, 128), fixed),
    ]
    operands = [proj, chan, shr, head]
    if dsc is not None:
        in_specs.append(pl.BlockSpec((CHUNK, width), tokens))
        operands.append(dsc)

    def body(*refs):
        forward_kernel(dsc is not None, *refs)

    return pl.pallas_call(
        body,
        name="mixer_forward",
        grid_spec=pltpu.PrefetchScalarGridSpec(
            num_scalar_prefetch=2,
            grid=(slots, count),
            in_specs=in_specs,
            out_specs=[
                pl.BlockSpec((CHUNK, width), tokens),
                pl.BlockSpec((CHUNK, width), tokens),
                pl.BlockSpec((1, STATE, width), in_order),
                pl.BlockSpec((1, 8, CHUNK), blocks),
            ],
            scratch_shapes=[
                pltpu.VMEM((CHUNK + 8, width), F32),
                pltpu.VMEM((CHUNK + 8, 2 * STATE), F32),
                pltpu.VMEM((STATE, width), F32),
            ],
        ),
        out_shape=[
            jax.ShapeDtypeStruct((rows, width), BF),
            jax.ShapeDtypeStruct((rows, width), BF),
            jax.ShapeDtypeStruct((slots * count, STATE, width), BF),
            jax.ShapeDtypeStruct((rows // CHUNK, 8, CHUNK), F32),
        ],
        compiler_params=pltpu.CompilerParams(vmem_limit_bytes=VMEM_LIMIT),
        cost_estimate=pl.CostEstimate(
            flops=rows * width * 1024, bytes_accessed=rows * width * 12, transcendentals=rows * width * 6
        ),
    )(v, lengths, *operands)


def mixer_backward(v, lengths, own_rows, proj, mixed, dsc, states, rates, chan, shr, head):
    rows = proj.shape[0]
    width = chan.shape[1]
    slots, count = rows // BUCKET, BUCKET // CHUNK
    place = chunk_index(own_rows, count)

    def tokens(slot, step, v_ref, len_ref):
        return (place(slot, count - 1 - step, v_ref[0]), 0)

    def tails(slot, step, v_ref, len_ref):
        previous = jnp.maximum(count - 2 - step, 0)
        return (place(slot, previous, v_ref[0]) * (CHUNK // 16) + CHUNK // 16 - 1, 0)

    def blocks(slot, step, v_ref, len_ref):
        return (place(slot, count - 1 - step, v_ref[0]), 0, 0)

    def in_order(slot, step, v_ref, len_ref):
        return (slot * count + count - 1 - step, 0, 0)

    def fixed(slot, step, v_ref, len_ref):
        return (0, 0)

    return pl.pallas_call(
        backward_kernel,
        name="mixer_backward",
        grid_spec=pltpu.PrefetchScalarGridSpec(
            num_scalar_prefetch=2,
            grid=(slots, count),
            in_specs=[
                pl.BlockSpec((CHUNK, proj.shape[1]), tokens),
                pl.BlockSpec((16, proj.shape[1]), tails),
                pl.BlockSpec((CHUNK, width), tokens),
                pl.BlockSpec((CHUNK, width), tokens),
                pl.BlockSpec((1, STATE, width), in_order),
                pl.BlockSpec((1, 8, CHUNK), blocks),
                pl.BlockSpec((8, width), fixed),
                pl.BlockSpec((8, 2 * STATE), fixed),
                pl.BlockSpec((8, 128), fixed),
            ],
            out_specs=[
                pl.BlockSpec((CHUNK, proj.shape[1]), tokens),
                pl.BlockSpec((CHUNK, width), tokens),
                pl.BlockSpec((8, width), fixed),
                pl.BlockSpec((8, 2 * STATE), fixed),
                pl.BlockSpec((8, 128), fixed),
            ],
            scratch_shapes=[
                pltpu.VMEM((CHUNK + 8, width), F32),
                pltpu.VMEM((CHUNK + 8, 2 * STATE), F32),
                pltpu.VMEM((CHUNK + 8, width), F32),
                pltpu.VMEM((CHUNK + 8, 2 * STATE), F32),
                pltpu.VMEM((STATE, width), F32),
                pltpu.VMEM((CHUNK, width), BF),
                pltpu.VMEM((CHUNK, width), BF),
            ],
        ),
        out_shape=[
            jax.ShapeDtypeStruct(proj.shape, BF),
            jax.ShapeDtypeStruct((rows, width), BF),
            jax.ShapeDtypeStruct((8, width), F32),
            jax.ShapeDtypeStruct((8, 2 * STATE), F32),
            jax.ShapeDtypeStruct((8, 128), F32),
        ],
        compiler_params=pltpu.CompilerParams(vmem_limit_bytes=VMEM_LIMIT),
        cost_estimate=pl.CostEstimate(
            flops=rows * width * 3072, bytes_accessed=rows * width * 20, transcendentals=rows * width * 10
        ),
    )(v, lengths, proj, proj, mixed, dsc, states, rates, chan, shr, head)


def xor_blocks(values, v):
    shape = values.shape
    values = values.reshape((2, 2, 2, shape[0] // 8) + shape[1:])
    for axis in range(3):
        bit = (v >> (2 - axis)) & 1
        values = jnp.where(bit == 1, jnp.flip(values, axis), values)
    return values.reshape(shape)


def flip_blocks(values, axis):
    shape = values.shape
    values = values.reshape((2, 2, 2, shape[0] // 8) + shape[1:])
    return jnp.flip(values, axis).reshape(shape)


def device(y, core, far, near, x):
    return (y * 2 + core) * 8 + far * 4 + near * 2 + x


def moves(where):
    found = []
    for place in itertools.product((0, 1), repeat=5):
        target = where(*place)
        if target is not None:
            found.append((device(*place), device(*target)))
    return found


FLIP_Y = moves(lambda y, c, f, n, x: (1 - y, c, f, n, x))
FLIP_CORE = moves(lambda y, c, f, n, x: (y, 1 - c, f, n, x))
FLIP_FAR = moves(lambda y, c, f, n, x: (y, c, 1 - f, n, x))
FLIP_NEAR = moves(lambda y, c, f, n, x: (y, c, f, 1 - n, x))
FLIP_X = moves(lambda y, c, f, n, x: (y, c, f, n, 1 - x))
SWAP = moves(lambda y, c, f, n, x: (y, f, c, n, x))
AWAY_Y = moves(lambda y, c, f, n, x: (1 - y, c, f, n, x) if c != f else None)
HOME_Y = moves(lambda y, c, f, n, x: (1 - y, c, f, n, x) if c == f else None)
TO_HOME = moves(lambda y, c, f, n, x: (y, c, c, n, x) if c != f else None)
HOME_CORE = moves(lambda y, c, f, n, x: (y, 1 - c, f, n, x) if c == f else None)


def send(values, perm):
    return lax.ppermute(values, AXES, perm)


class Square:
    def __init__(self):
        dp, mp = lax.axis_index("dp"), lax.axis_index("mp")
        core, self.y, far = dp % 2, dp // 2, mp // 4
        self.v = (core * 4 + mp % 4).astype(jnp.int32)
        self.home = core == far

    def swap(self, values):
        return send(values, SWAP)

    def fetch(self, values):
        half = values.shape[0] // 2
        got = send(lax.dynamic_slice_in_dim(values, self.y * half, half, 0), SWAP)
        other = send(got, AWAY_Y)
        first = jnp.where(self.y == 0, got, other)
        second = jnp.where(self.y == 0, other, got)
        return jnp.where(self.home, values, jnp.concatenate([first, second], axis=0))

    def gather(self, own):
        half = own.shape[0] // 2
        side, up = send(own, FLIP_X), send(own, FLIP_NEAR)
        first, second = send(up[:half], FLIP_X), send(side[half:], FLIP_NEAR)
        blocks = [own, side, up, jnp.concatenate([first, second], axis=0)]
        return jnp.concatenate(blocks + [send(item, FLIP_CORE) for item in blocks], axis=0)

    def scatter(self, rows, make):
        n = rows // 8
        half = n // 2
        other = send(make(slice(4 * n, 8 * n)), FLIP_CORE)
        here = make(slice(0, 4 * n))

        def block(r, part=slice(0, n)):
            at = slice(r * n + part.start, r * n + part.stop)
            return here[at].astype(F32) + other[at].astype(F32)

        top, bottom = slice(0, half), slice(half, n)
        first = send(block(3, top).astype(BF), FLIP_X)
        second = send(block(3, bottom).astype(BF), FLIP_NEAR)
        side = [block(1, top).astype(BF), (block(1, bottom) + second.astype(F32)).astype(BF)]
        up = [(block(2, top) + first.astype(F32)).astype(BF), block(2, bottom).astype(BF)]
        side = [send(item, FLIP_X) for item in side]
        up = [send(item, FLIP_NEAR) for item in up]
        return jnp.concatenate(
            [
                block(0, part) + side[i].astype(F32) + up[i].astype(F32)
                for i, part in enumerate((top, bottom))
            ],
            axis=0,
        )

    def sum_rows(self, values):
        for axis, perm in enumerate((FLIP_CORE, FLIP_NEAR, FLIP_X)):
            values = values + flip_blocks(send(values, perm), axis)
        return values

    def own(self, values):
        return values[: values.shape[0] // 8]

    def reduce_weight(self, part):
        half = part.shape[0] // 2
        low = part.astype(BF)
        keep = jnp.where(self.y == 0, part[:half], part[half:])
        away = jnp.where(self.y == 0, low[half:], low[:half])
        mine = (keep + send(away, FLIP_Y).astype(F32)).astype(BF)
        total = (mine.astype(F32) + send(mine, TO_HOME).astype(F32)).astype(BF)
        other = send(total, HOME_Y)
        whole = jnp.concatenate(
            [jnp.where(self.y == 0, total, other), jnp.where(self.y == 0, other, total)], axis=0
        )
        return jnp.where(self.home, whole, send(whole, HOME_CORE)).astype(F32)

    def reduce_heads(self, part):
        part = part + send(part, FLIP_Y)
        part = part + send(part, TO_HOME)
        return jnp.where(self.home, part, send(part, HOME_CORE))

    def reduce_all(self, part):
        for perm in (FLIP_Y, FLIP_FAR, FLIP_X, FLIP_NEAR, FLIP_CORE):
            part = part + send(part, perm)
        return part

    def reduce_shared(self, part):
        part = xor_blocks(part.astype(BF), self.v)
        own = self.scatter(part.shape[0], lambda at: part[at])
        own = own + send(own, FLIP_Y)
        own = own + send(own, FLIP_FAR)
        return xor_blocks(self.gather(own.astype(BF)), self.v).astype(F32)


class Straight:
    def __init__(self):
        self.v = jnp.int32(0)

    def swap(self, values):
        return values

    fetch = swap

    def gather(self, own):
        return lax.all_gather(own, "mp", axis=0, tiled=True)

    def scatter(self, rows, make):
        part = make(slice(0, rows))
        return lax.psum_scatter(part, "mp", scatter_dimension=0, tiled=True).astype(F32)

    def sum_rows(self, values):
        return lax.psum(values, "mp")

    def own(self, values):
        count = values.shape[0] // lax.axis_size("mp")
        return lax.dynamic_slice_in_dim(values, lax.axis_index("mp") * count, count, 0)

    def reduce_weight(self, part):
        return lax.psum(part.astype(BF), "dp").astype(F32)

    def reduce_heads(self, part):
        return lax.psum(part, "dp")

    def reduce_all(self, part):
        return lax.psum(part, AXES)

    reduce_shared = reduce_all


def local(
    hidden,
    lengths,
    pre_gain,
    w_inner,
    w_step,
    w_shared,
    conv_inner,
    conv_inner_bias,
    conv_shared,
    conv_shared_bias,
    step_bias,
    decay_log,
    skip_gain,
    norm_gain,
    w_out,
    out_grad,
):
    square = lax.axis_size("dp") == 4 and lax.axis_size("mp") == 8 and lengths.shape[0] == 1
    comm = Square() if square else Straight()
    own_rows, features = hidden.shape
    group_rows = lengths.shape[0] * BUCKET
    width = w_inner.shape[3]
    heads = w_step.shape[2]
    total_width = width * lax.axis_size("mp")
    v = comm.v.reshape(1)

    state_low = comm.swap(hidden)
    decay = -jnp.exp(decay_log)
    chan = jnp.concatenate(
        [
            conv_inner,
            conv_inner_bias[:, None],
            norm_gain[:, None],
            jnp.repeat(skip_gain, HEAD_DIM, axis=1)[:, None],
            jnp.zeros((LAYERS, 1, width), F32),
        ],
        axis=1,
    )
    lane_pad = ((0, 0), (0, 0), (0, 128 - heads))
    head = jnp.pad(jnp.stack([step_bias, decay], axis=1), ((0, 0), (0, 6), (0, 128 - heads)))
    chan, head, live = comm.swap(chan), comm.swap(head), comm.swap(lengths)
    steps = jnp.pad(comm.swap(w_step), lane_pad)
    shr = jnp.concatenate(
        [conv_shared, conv_shared_bias[:, None], jnp.zeros((LAYERS, 3, 2 * STATE), F32)], axis=1
    )
    inner, outer = [], []
    for depth in range(LAYERS):
        fetched = comm.fetch(w_inner[depth]).reshape(features, 2 * width)
        inner.append(jnp.concatenate([fetched, w_shared[depth], steps[depth]], axis=1))
        outer.append(comm.fetch(w_out[depth]))
    last_low = comm.swap(out_grad)

    state = state_low.astype(F32)
    saved = []
    branches = []
    sums = None
    for depth in range(LAYERS):
        scale_pre = lax.rsqrt(jnp.mean(state * state, axis=-1, keepdims=True) + EPSILON)
        base = state * scale_pre
        normed = comm.gather((base * pre_gain[depth]).astype(BF))
        proj = mm(normed, inner[depth]).astype(BF)
        g_full = dsc = None
        if depth == LAYERS - 1:
            g_full = comm.gather(last_low)
            dsc = mm(g_full, outer[depth], ((1,), (1,))).astype(BF)
        tall, mixed, states, sums = mixer_forward(
            v, live, own_rows, proj, chan[depth], shr[depth], head[depth], dsc
        )
        sums = comm.sum_rows(sums[:, 0:2])
        ratio = lax.rsqrt(sums[:, 0] / total_width + EPSILON)
        own_ratio = comm.own(ratio).reshape(own_rows, 1)
        branch = own_ratio * comm.scatter(
            group_rows, lambda at: mm(tall[at], outer[depth]).astype(BF)
        )
        branches.append(branch)
        state = state + branch
        saved.append((base, scale_pre, normed, proj, mixed, states, ratio, g_full, dsc))

    carried = last_low.astype(F32)
    change = 0.0
    wide, heads_part, all_part = [None] * LAYERS, [None] * LAYERS, [None] * LAYERS
    for depth in reversed(range(LAYERS)):
        base, scale_pre, normed, proj, mixed, states, ratio, g_full, dsc = saved[depth]
        if depth == LAYERS - 1:
            pull = ratio * ratio * ratio * sums[:, 1] / total_width
        else:
            g_low = carried.astype(BF)
            cross = jnp.sum(g_low.astype(F32) * branches[depth], axis=1)
            cross = comm.gather(cross.reshape(own_rows // CHUNK, CHUNK))
            pull = ratio * ratio * cross / total_width
            g_full = comm.gather(g_low)
            dsc = mm(g_full, outer[depth], ((1,), (1,))).astype(BF)
        rates = jnp.pad(jnp.stack([ratio, pull], axis=1), ((0, 0), (0, 6), (0, 0)))
        low, scaled, g_chan, g_shr, g_head = mixer_backward(
            v, live, own_rows, proj, mixed, dsc, states, rates, chan[depth], shr[depth], head[depth]
        )
        d_normed = comm.scatter(
            group_rows, lambda at: mm(low[at], inner[depth], ((1,), (1,))).astype(BF)
        )
        g_outer = comm.reduce_weight(mm(scaled, g_full, ((0,), (0,))))
        g_inner = mm(normed, low, ((0,), (0,)))
        g_gate = comm.reduce_weight(g_inner[:, :width])
        g_raw = comm.reduce_weight(g_inner[:, width : 2 * width])
        g_shared = comm.reduce_shared(g_inner[:, 2 * width : 2 * width + 2 * STATE])
        g_step = g_inner[:, 2 * width + 2 * STATE : 2 * width + 2 * STATE + heads].T
        wide[depth] = (jnp.stack([g_gate, g_raw], axis=1), g_outer, g_shared)
        g_pre = jnp.sum(d_normed * base, axis=0)
        d_base = d_normed * pre_gain[depth]
        moved = scale_pre * (d_base - base * jnp.mean(d_base * base, axis=-1, keepdims=True))
        carried = carried + moved
        change = change + moved
        heads_part[depth] = jnp.concatenate(
            [g_step.reshape(-1, 128), g_chan.reshape(-1, 128), g_head], axis=0
        )
        all_part[depth] = jnp.concatenate([g_pre.reshape(-1, 128), g_shr.reshape(-1, 128)], axis=0)

    first_out = hidden.astype(F32) + comm.swap(branches[0].astype(BF)).astype(F32)
    second_out = first_out + comm.swap(branches[1].astype(BF)).astype(F32)
    hidden_grad = out_grad.astype(F32) + comm.swap(change.astype(BF)).astype(F32)
    per_head = comm.reduce_heads(jnp.stack(heads_part))
    everywhere = comm.reduce_all(jnp.stack(all_part))
    step_rows, chan_rows = heads * features // 128, 8 * width // 128
    g_step = per_head[:, :step_rows].reshape(LAYERS, heads, features).transpose(0, 2, 1)
    g_chan = per_head[:, step_rows : step_rows + chan_rows].reshape(LAYERS, 8, width)
    g_head = per_head[:, step_rows + chan_rows :]
    pre_rows = features // 128
    g_pre = everywhere[:, :pre_rows].reshape(LAYERS, features)
    g_shr = everywhere[:, pre_rows:].reshape(LAYERS, 8, 2 * STATE)
    return (
        first_out,
        second_out,
        hidden_grad,
        g_pre,
        jnp.stack([item[0] for item in wide]),
        g_step,
        jnp.stack([item[2] for item in wide]),
        g_chan[:, 0:4],
        g_chan[:, 4],
        g_shr[:, 0:4],
        g_shr[:, 4],
        g_head[:, 0, :heads],
        g_head[:, 1, :heads] * decay,
        g_chan[:, 6].reshape(LAYERS, heads, HEAD_DIM).sum(axis=-1),
        g_chan[:, 5],
        jnp.stack([item[1] for item in wide]),
    )


def solution(mesh):
    placed = (
        P(("dp", "mp"), None),
        P("dp"),
        P(),
        P(None, None, None, "mp"),
        P(None, None, "mp"),
        P(),
        P(None, None, "mp"),
        P(None, "mp"),
        P(),
        P(),
        P(None, "mp"),
        P(None, "mp"),
        P(None, "mp"),
        P(None, "mp"),
        P(None, "mp", None),
        P(("dp", "mp"), None),
    )
    return jax.shard_map(
        local,
        mesh=mesh,
        in_specs=placed,
        out_specs=(
            P(("dp", "mp"), None),
            P(("dp", "mp"), None),
            P(("dp", "mp"), None),
            P(),
            P(None, None, None, "mp"),
            P(None, None, "mp"),
            P(),
            P(None, None, "mp"),
            P(None, "mp"),
            P(),
            P(),
            P(None, "mp"),
            P(None, "mp"),
            P(None, "mp"),
            P(None, "mp"),
            P(None, "mp", None),
        ),
        check_vma=False,
    )
```

```python
import itertools
import math

import jax
import jax.numpy as jnp
from jax import lax
from jax.experimental import pallas as pl
from jax.experimental.pallas import tpu as pltpu
from jax.sharding import PartitionSpec as P

HEAD_DIM = 64
STATE = 128
BUCKET = 2048
LAYERS = 2
CHUNK = 128
SMALL = 3 * STATE
EPSILON = 1e-05
LOG2E = math.log2(math.e)
VMEM_LIMIT = 56 << 20
AXES = ("dp", "mp")
BF = jnp.bfloat16
F32 = jnp.float32


def mm(a, b, dims=((1,), (0,))):
    return lax.dot_general(a, b, (dims, ((), ())), preferred_element_type=F32)


def mm_exact(a, b, dims=((1,), (0,))):
    return lax.dot_general(
        a, b, (dims, ((), ())), preferred_element_type=F32, precision=lax.Precision.HIGHEST
    )


def mm_split(a, ones):
    high = a.astype(BF)
    return mm(high, ones) + mm((a - high.astype(F32)).astype(BF), ones)


def sigmoid(v):
    return 0.5 * jnp.tanh(0.5 * v) + 0.5


def iota(shape, axis):
    return lax.broadcasted_iota(jnp.int32, shape, axis)


def softplus(v):
    return jnp.maximum(v, 0.0) + jnp.log1p(jnp.exp(-jnp.abs(v)))


def step_terms(step_raw, head_ref, lower):
    shifted = step_raw + head_ref[0:1, :]
    delta = softplus(shifted)
    logs = mm_exact(lower, delta * (head_ref[1:2, :] * LOG2E))
    return shifted, delta, logs, logs.T


def column(values, head):
    return jnp.broadcast_to(values[:, head : head + 1], (values.shape[0], 128))


def forward_kernel(cross, v_ref, len_ref, *refs):
    if cross:
        proj_ref, chan_ref, shr_ref, head_ref, dsc_ref, *refs = refs
    else:
        proj_ref, chan_ref, shr_ref, head_ref, *refs = refs
    h_ref, mixed_ref, st_ref, sums_ref, raw_buf, shr_buf, state = refs
    width = h_ref.shape[1]
    length = CHUNK
    chunk = pl.program_id(1)

    @pl.when(chunk == 0)
    def _():
        raw_buf[0:8, :] = jnp.zeros((8, width), F32)
        shr_buf[0:8, :] = jnp.zeros((8, 2 * STATE), F32)
        state[...] = jnp.zeros_like(state)

    mask = (chunk * length + iota((length, 128), 0) < len_ref[pl.program_id(0)]).astype(F32)
    row, col = iota((length, length), 0), iota((length, length), 1)
    lower = row >= col
    low_half = iota((length, 128), 1) < HEAD_DIM

    shr_buf[8 : 8 + length, :] = proj_ref[:, 2 * width : 2 * width + 2 * STATE].astype(F32)
    parts = []
    for part in range(2):
        lanes = slice(part * STATE, (part + 1) * STATE)
        pre = shr_ref[4:5, lanes] + shr_ref[0:1, lanes] * shr_buf[8 : 8 + length, lanes]
        for lag in range(1, 4):
            pre = pre + shr_ref[lag : lag + 1, lanes] * shr_buf[8 - lag : 8 - lag + length, lanes]
        parts.append((pre * sigmoid(pre) * mask).astype(BF))
    b_low, c_low = parts
    shr_buf[0:8, :] = shr_buf[length : length + 8, :]
    scores = mm(c_low, b_low, ((1,), (1,)))

    step_raw = proj_ref[:, 2 * width + 2 * STATE : 2 * width + 3 * STATE].astype(F32)
    _, delta, logs, logs_t = step_terms(step_raw, head_ref, lower.astype(F32))

    raw_buf[8 : 8 + length, :] = proj_ref[:, width : 2 * width].astype(F32)
    state_low = state[...].astype(BF)
    st_ref[0] = state_low
    ones = jnp.ones((8, 128), BF)
    square = jnp.zeros((8, length), F32)
    crossing = jnp.zeros((8, length), F32)
    for pair in range(width // 128):
        lanes = slice(pair * 128, pair * 128 + 128)
        pre = chan_ref[4:5, lanes] + chan_ref[0:1, lanes] * raw_buf[8 : 8 + length, lanes]
        for lag in range(1, 4):
            pre = pre + chan_ref[lag : lag + 1, lanes] * raw_buf[8 - lag : 8 - lag + length, lanes]
        x = pre * sigmoid(pre) * mask
        cols = (column(logs, 2 * pair), column(logs, 2 * pair + 1))
        logs_pair = jnp.where(low_half, cols[0], cols[1])
        u = x * jnp.where(low_half, column(delta, 2 * pair), column(delta, 2 * pair + 1))
        weights = []
        for half in range(2):
            head = 2 * pair + half
            gap = jnp.where(lower, cols[half] - logs_t[head : head + 1, :], -1e30)
            weights.append((scores * jnp.exp2(gap)).astype(BF))
        u_low = u.astype(BF)
        zero = jnp.zeros_like(u_low)
        direct = mm(
            jnp.concatenate(weights, axis=1),
            jnp.concatenate([jnp.where(low_half, u_low, zero), jnp.where(low_half, zero, u_low)], axis=0),
        )
        carried = mm(c_low, state_low[:, lanes])
        mixed = direct + jnp.exp2(logs_pair) * carried + chan_ref[6:7, lanes] * x
        mixed_ref[:, lanes] = mixed.astype(BF)
        total = logs_pair[length - 1 : length, :]
        fresh = mm(b_low, (u * jnp.exp2(total - logs_pair)).astype(BF), ((0,), (0,)))
        state[:, lanes] = state[:, lanes] * jnp.exp2(total) + fresh
        gate = proj_ref[:, lanes].astype(F32)
        gated = mixed * (gate * sigmoid(gate))
        scaled = gated * chan_ref[5:6, lanes]
        h_ref[:, lanes] = scaled.astype(BF)
        square = square + mm(ones, (gated * gated).astype(BF), ((1,), (1,)))
        if cross:
            product = dsc_ref[:, lanes].astype(F32) * scaled
            high = product.astype(BF)
            rest = (product - high.astype(F32)).astype(BF)
            crossing = crossing + mm(ones, high, ((1,), (1,))) + mm(ones, rest, ((1,), (1,)))
    raw_buf[0:8, :] = raw_buf[length : length + 8, :]
    sums_ref[0] = jnp.where(iota((8, length), 0) == 0, square, crossing)


def backward_kernel(v_ref, len_ref, *refs):
    (proj_ref, tail_ref, mixed_ref, dsc_ref, st_ref, rat_ref, chan_ref, shr_ref, head_ref) = refs[:9]
    (low_ref, scaled_ref, g_chan_ref, g_shr_ref, g_head_ref) = refs[9:14]
    (raw_buf, shr_buf, dpre_buf, dshr_buf, d_state, u_all, ey_all) = refs[14:]
    width = mixed_ref.shape[1]
    pairs = width // 128
    length = CHUNK
    step = pl.program_id(1)
    chunk = pl.num_programs(1) - 1 - step

    @pl.when(step == 0)
    def _():
        dpre_buf[length : length + 8, :] = jnp.zeros((8, width), F32)
        dshr_buf[length : length + 8, :] = jnp.zeros((8, 2 * STATE), F32)
        d_state[...] = jnp.zeros_like(d_state)

    @pl.when((step == 0) & (pl.program_id(0) == 0))
    def _():
        g_chan_ref[...] = jnp.zeros_like(g_chan_ref)
        g_shr_ref[...] = jnp.zeros_like(g_shr_ref)
        g_head_ref[...] = jnp.zeros_like(g_head_ref)

    mask = (chunk * length + iota((length, 128), 0) < len_ref[pl.program_id(0)]).astype(F32)
    row, col = iota((length, length), 0), iota((length, length), 1)
    lower = row >= col
    lower_f = lower.astype(F32)
    upper_f = (row <= col).astype(F32)
    strict_f = (row > col).astype(F32)
    lane = iota((length, 128), 1)
    low_half = lane < HEAD_DIM
    inside = (chunk > 0).astype(F32)

    shr_buf[0:8, :] = tail_ref[8:16, 2 * width : 2 * width + 2 * STATE].astype(F32) * inside
    shr_buf[8 : 8 + length, :] = proj_ref[:, 2 * width : 2 * width + 2 * STATE].astype(F32)
    parts, slopes = [], []
    for part in range(2):
        lanes = slice(part * STATE, (part + 1) * STATE)
        pre = shr_ref[4:5, lanes] + shr_ref[0:1, lanes] * shr_buf[8 : 8 + length, lanes]
        for lag in range(1, 4):
            pre = pre + shr_ref[lag : lag + 1, lanes] * shr_buf[8 - lag : 8 - lag + length, lanes]
        s = sigmoid(pre)
        value = pre * s
        parts.append((value * mask).astype(BF))
        slopes.append(mask * (s + value * (1.0 - s)))
    b_low, c_low = parts
    scores = mm(c_low, b_low, ((1,), (1,)))

    step_raw = proj_ref[:, 2 * width + 2 * STATE : 2 * width + 3 * STATE].astype(F32)
    shifted, delta, logs, logs_t = step_terms(step_raw, head_ref, lower_f)
    scales = rat_ref[0].T
    ratio = jnp.broadcast_to(scales[:, 0:1], (length, 128))
    pull = jnp.broadcast_to(scales[:, 1:2], (length, 128))

    raw_buf[0:8, :] = tail_ref[8:16, width : 2 * width].astype(F32) * inside
    raw_buf[8 : 8 + length, :] = proj_ref[:, width : 2 * width].astype(F32)

    d_scores = jnp.zeros((length, length), F32)
    rows_sum = jnp.zeros((length, 128), F32)
    cols_sum = jnp.zeros((8, length), F32)
    before = jnp.zeros((length, 128), F32)
    after = jnp.zeros((length, 128), F32)
    d_delta = jnp.zeros((length, 128), F32)
    leaving = jnp.zeros((8, 128), F32)
    for pair in range(pairs):
        lanes = slice(pair * 128, pair * 128 + 128)
        heads = (iota((128, 128), 1) == 2 * pair + iota((128, 128), 0) // HEAD_DIM).astype(BF)
        gain = chan_ref[5:6, lanes]
        gate = proj_ref[:, lanes].astype(F32)
        mixed = mixed_ref[:, lanes].astype(F32)
        dsc = dsc_ref[:, lanes].astype(F32)
        s = sigmoid(gate)
        swish = gate * s
        gated = mixed * swish
        unit = gated * ratio
        g_chan_ref[5:6, lanes] += jnp.sum(dsc * unit, axis=0, keepdims=True)
        scaled_ref[:, lanes] = (unit * gain).astype(BF)
        d_gated = ratio * (dsc * gain) - gated * pull
        dy = d_gated * swish
        low_ref[:, lanes] = (d_gated * mixed * (s + swish * (1.0 - s))).astype(BF)
        pre = chan_ref[4:5, lanes] + chan_ref[0:1, lanes] * raw_buf[8 : 8 + length, lanes]
        for lag in range(1, 4):
            pre = pre + chan_ref[lag : lag + 1, lanes] * raw_buf[8 - lag : 8 - lag + length, lanes]
        s = sigmoid(pre)
        value = pre * s
        x = value * mask
        slope = mask * (s + value * (1.0 - s))
        g_chan_ref[6:7, lanes] += jnp.sum(dy * x, axis=0, keepdims=True)
        cols = (column(logs, 2 * pair), column(logs, 2 * pair + 1))
        logs_pair = jnp.where(low_half, cols[0], cols[1])
        delta_pair = jnp.where(low_half, column(delta, 2 * pair), column(delta, 2 * pair + 1))
        u = x * delta_pair
        u_low = u.astype(BF)
        dy_low = dy.astype(BF)
        zero = jnp.zeros_like(dy_low)
        dy_two = jnp.concatenate(
            [jnp.where(low_half, dy_low, zero), jnp.where(low_half, zero, dy_low)], axis=0
        )
        d_weights = mm(dy_two, u_low, ((1,), (1,)))
        weights = []
        for half in range(2):
            head = 2 * pair + half
            fade = jnp.exp2(jnp.where(lower, cols[half] - logs_t[head : head + 1, :], -1e30))
            weights.append((scores * fade).astype(BF))
            pulled = d_weights[half * length : (half + 1) * length, :] * fade
            d_scores = d_scores + pulled
            moved = pulled * scores
            rows_sum = jnp.where(lane == head, jnp.sum(moved, axis=1, keepdims=True), rows_sum)
            cols_sum = jnp.where(
                iota((8, length), 0) == head, jnp.sum(moved, axis=0, keepdims=True), cols_sum
            )
        d_u = mm(jnp.concatenate(weights, axis=0), dy_two, ((0,), (0,)))
        rise = jnp.exp2(logs_pair)
        total = logs_pair[length - 1 : length, :]
        fall = jnp.exp2(total - logs_pair)
        state_low = st_ref[0, :, lanes]
        d_next = d_state[:, lanes]
        d_next_low = d_next.astype(BF)
        e_dy = dy * rise
        e_low = e_dy.astype(BF)
        ey_all[:, lanes] = e_low
        u_all[:, lanes] = (u * fall).astype(BF)
        rows_sum = rows_sum + mm_split(e_dy * mm(c_low, state_low), heads)
        through = fall * mm(b_low, d_next_low)
        before = before + mm_split(u * through, heads)
        d_u = d_u + through
        d_delta = d_delta + mm_split(x * d_u, heads)
        whole = jnp.exp2(total)
        kept = jnp.sum(state_low.astype(F32) * d_next, axis=0, keepdims=True) * whole
        leaving = leaving + mm_split(jnp.broadcast_to(kept, (8, 128)), heads)
        d_state[:, lanes] = d_next * whole + mm(c_low, e_low, ((0,), (0,)))
        after = after + mm(e_low, state_low, ((1,), (1,)))
        shr_part = mm(u_all[:, lanes], d_next_low, ((1,), (1,)))
        if pair == 0:
            d_b = shr_part
        else:
            d_b = d_b + shr_part
        d_x = delta_pair * d_u + chan_ref[6:7, lanes] * dy
        d_pre = d_x * slope
        dpre_buf[0:length, lanes] = d_pre
        g_chan_ref[4:5, lanes] += jnp.sum(d_pre, axis=0, keepdims=True)
        d_raw = chan_ref[0:1, lanes] * d_pre
        g_chan_ref[0:1, lanes] += jnp.sum(d_pre * raw_buf[8 : 8 + length, lanes], axis=0, keepdims=True)
        for lag in range(1, 4):
            d_raw = d_raw + chan_ref[lag : lag + 1, lanes] * dpre_buf[lag : lag + length, lanes]
            g_chan_ref[lag : lag + 1, lanes] += jnp.sum(
                d_pre * raw_buf[8 - lag : 8 - lag + length, lanes], axis=0, keepdims=True
            )
        low_ref[:, width + pair * 128 : width + pair * 128 + 128] = d_raw.astype(BF)
    dpre_buf[length : length + 8, :] = dpre_buf[0:8, :]

    ds_low = d_scores.astype(BF)
    d_b = d_b + mm(ds_low, c_low, ((0,), (0,)))
    d_c = after + mm(ds_low, b_low)
    for part, value in enumerate((d_b, d_c)):
        lanes = slice(part * STATE, (part + 1) * STATE)
        d_pre = value * slopes[part]
        dshr_buf[0:length, lanes] = d_pre
        g_shr_ref[4:5, lanes] += jnp.sum(d_pre, axis=0, keepdims=True)
        d_raw = shr_ref[0:1, lanes] * d_pre
        g_shr_ref[0:1, lanes] += jnp.sum(d_pre * shr_buf[8 : 8 + length, lanes], axis=0, keepdims=True)
        for lag in range(1, 4):
            d_raw = d_raw + shr_ref[lag : lag + 1, lanes] * dshr_buf[lag : lag + length, lanes]
            g_shr_ref[lag : lag + 1, lanes] += jnp.sum(
                d_pre * shr_buf[8 - lag : 8 - lag + length, lanes], axis=0, keepdims=True
            )
        low_ref[:, 2 * width + part * STATE : 2 * width + (part + 1) * STATE] = d_raw.astype(BF)
    dshr_buf[length : length + 8, :] = dshr_buf[0:8, :]

    cols_all = jnp.concatenate([cols_sum, jnp.zeros((length - 8, length), F32)], axis=0)
    d_log = (
        mm_exact(upper_f, rows_sum)
        - mm_exact(upper_f, cols_all, ((1,), (1,)))
        + mm_exact(strict_f, before)
        + leaving[0:1, :]
    )
    d_delta = d_delta + head_ref[1:2, :] * d_log
    d_step = d_delta * sigmoid(shifted)
    low_ref[:, 2 * width + 2 * STATE : 2 * width + 3 * STATE] = d_step.astype(BF)
    g_head_ref[0:1, :] += jnp.sum(d_step, axis=0, keepdims=True)
    g_head_ref[1:2, :] += jnp.sum(delta * d_log, axis=0, keepdims=True)


def chunk_index(own_rows, count):
    per_block = own_rows // CHUNK

    def place(slot, chunk, v):
        return slot * count + ((chunk // per_block) ^ v) * per_block + chunk % per_block

    return place


def mixer_forward(v, lengths, own_rows, proj, chan, shr, head, dsc=None):
    rows = proj.shape[0]
    width = chan.shape[1]
    slots, count = rows // BUCKET, BUCKET // CHUNK
    place = chunk_index(own_rows, count)

    def tokens(slot, chunk, v_ref, len_ref):
        return (place(slot, chunk, v_ref[0]), 0)

    def blocks(slot, chunk, v_ref, len_ref):
        return (place(slot, chunk, v_ref[0]), 0, 0)

    def fixed(slot, chunk, v_ref, len_ref):
        return (0, 0)

    def in_order(slot, chunk, v_ref, len_ref):
        return (slot * count + chunk, 0, 0)

    in_specs = [
        pl.BlockSpec((CHUNK, proj.shape[1]), tokens),
        pl.BlockSpec((8, width), fixed),
        pl.BlockSpec((8, 2 * STATE), fixed),
        pl.BlockSpec((8, 128), fixed),
    ]
    operands = [proj, chan, shr, head]
    if dsc is not None:
        in_specs.append(pl.BlockSpec((CHUNK, width), tokens))
        operands.append(dsc)

    def body(*refs):
        forward_kernel(dsc is not None, *refs)

    return pl.pallas_call(
        body,
        name="mixer_forward",
        grid_spec=pltpu.PrefetchScalarGridSpec(
            num_scalar_prefetch=2,
            grid=(slots, count),
            in_specs=in_specs,
            out_specs=[
                pl.BlockSpec((CHUNK, width), tokens),
                pl.BlockSpec((CHUNK, width), tokens),
                pl.BlockSpec((1, STATE, width), in_order),
                pl.BlockSpec((1, 8, CHUNK), blocks),
            ],
            scratch_shapes=[
                pltpu.VMEM((CHUNK + 8, width), F32),
                pltpu.VMEM((CHUNK + 8, 2 * STATE), F32),
                pltpu.VMEM((STATE, width), F32),
            ],
        ),
        out_shape=[
            jax.ShapeDtypeStruct((rows, width), BF),
            jax.ShapeDtypeStruct((rows, width), BF),
            jax.ShapeDtypeStruct((slots * count, STATE, width), BF),
            jax.ShapeDtypeStruct((rows // CHUNK, 8, CHUNK), F32),
        ],
        compiler_params=pltpu.CompilerParams(vmem_limit_bytes=VMEM_LIMIT),
        cost_estimate=pl.CostEstimate(
            flops=rows * width * 1024, bytes_accessed=rows * width * 12, transcendentals=rows * width * 6
        ),
    )(v, lengths, *operands)


def mixer_backward(v, lengths, own_rows, proj, mixed, dsc, states, rates, chan, shr, head):
    rows = proj.shape[0]
    width = chan.shape[1]
    slots, count = rows // BUCKET, BUCKET // CHUNK
    place = chunk_index(own_rows, count)

    def tokens(slot, step, v_ref, len_ref):
        return (place(slot, count - 1 - step, v_ref[0]), 0)

    def tails(slot, step, v_ref, len_ref):
        previous = jnp.maximum(count - 2 - step, 0)
        return (place(slot, previous, v_ref[0]) * (CHUNK // 16) + CHUNK // 16 - 1, 0)

    def blocks(slot, step, v_ref, len_ref):
        return (place(slot, count - 1 - step, v_ref[0]), 0, 0)

    def in_order(slot, step, v_ref, len_ref):
        return (slot * count + count - 1 - step, 0, 0)

    def fixed(slot, step, v_ref, len_ref):
        return (0, 0)

    return pl.pallas_call(
        backward_kernel,
        name="mixer_backward",
        grid_spec=pltpu.PrefetchScalarGridSpec(
            num_scalar_prefetch=2,
            grid=(slots, count),
            in_specs=[
                pl.BlockSpec((CHUNK, proj.shape[1]), tokens),
                pl.BlockSpec((16, proj.shape[1]), tails),
                pl.BlockSpec((CHUNK, width), tokens),
                pl.BlockSpec((CHUNK, width), tokens),
                pl.BlockSpec((1, STATE, width), in_order),
                pl.BlockSpec((1, 8, CHUNK), blocks),
                pl.BlockSpec((8, width), fixed),
                pl.BlockSpec((8, 2 * STATE), fixed),
                pl.BlockSpec((8, 128), fixed),
            ],
            out_specs=[
                pl.BlockSpec((CHUNK, proj.shape[1]), tokens),
                pl.BlockSpec((CHUNK, width), tokens),
                pl.BlockSpec((8, width), fixed),
                pl.BlockSpec((8, 2 * STATE), fixed),
                pl.BlockSpec((8, 128), fixed),
            ],
            scratch_shapes=[
                pltpu.VMEM((CHUNK + 8, width), F32),
                pltpu.VMEM((CHUNK + 8, 2 * STATE), F32),
                pltpu.VMEM((CHUNK + 8, width), F32),
                pltpu.VMEM((CHUNK + 8, 2 * STATE), F32),
                pltpu.VMEM((STATE, width), F32),
                pltpu.VMEM((CHUNK, width), BF),
                pltpu.VMEM((CHUNK, width), BF),
            ],
        ),
        out_shape=[
            jax.ShapeDtypeStruct(proj.shape, BF),
            jax.ShapeDtypeStruct((rows, width), BF),
            jax.ShapeDtypeStruct((8, width), F32),
            jax.ShapeDtypeStruct((8, 2 * STATE), F32),
            jax.ShapeDtypeStruct((8, 128), F32),
        ],
        compiler_params=pltpu.CompilerParams(vmem_limit_bytes=VMEM_LIMIT),
        cost_estimate=pl.CostEstimate(
            flops=rows * width * 3072, bytes_accessed=rows * width * 20, transcendentals=rows * width * 10
        ),
    )(v, lengths, proj, proj, mixed, dsc, states, rates, chan, shr, head)


def xor_blocks(values, v):
    shape = values.shape
    values = values.reshape((2, 2, 2, shape[0] // 8) + shape[1:])
    for axis in range(3):
        bit = (v >> (2 - axis)) & 1
        values = jnp.where(bit == 1, jnp.flip(values, axis), values)
    return values.reshape(shape)


def flip_blocks(values, axis):
    shape = values.shape
    values = values.reshape((2, 2, 2, shape[0] // 8) + shape[1:])
    return jnp.flip(values, axis).reshape(shape)


def device(y, core, far, near, x):
    return (y * 2 + core) * 8 + far * 4 + near * 2 + x


def moves(where):
    found = []
    for place in itertools.product((0, 1), repeat=5):
        target = where(*place)
        if target is not None and target != place:
            found.append((device(*place), device(*target)))
    return found


FLIP_Y = moves(lambda y, c, f, n, x: (1 - y, c, f, n, x))
FLIP_CORE = moves(lambda y, c, f, n, x: (y, 1 - c, f, n, x))
FLIP_FAR = moves(lambda y, c, f, n, x: (y, c, 1 - f, n, x))
FLIP_NEAR = moves(lambda y, c, f, n, x: (y, c, f, 1 - n, x))
FLIP_X = moves(lambda y, c, f, n, x: (y, c, f, n, 1 - x))
SWAP = moves(lambda y, c, f, n, x: (y, f, c, n, x))
AWAY_Y = moves(lambda y, c, f, n, x: (1 - y, c, f, n, x) if c != f else None)
HOME_Y = moves(lambda y, c, f, n, x: (1 - y, c, f, n, x) if c == f else None)
TO_HOME = moves(lambda y, c, f, n, x: (y, c, c, n, x) if c != f else None)
HOME_CORE = moves(lambda y, c, f, n, x: (y, 1 - c, f, n, x) if c == f else None)


def send(values, perm):
    return lax.ppermute(values, AXES, perm)


def neighbours():
    dp, mp = lax.axis_index("dp"), lax.axis_index("mp")
    x = (dp, mp + 1 - 2 * (mp % 2))
    near = (dp, mp + 2 - 4 * ((mp // 2) % 2))
    core = (dp + 1 - 2 * (dp % 2), mp)
    return x, near, core


def greet(targets):
    barrier = pltpu.get_barrier_semaphore()
    for target in targets:
        pl.semaphore_signal(barrier, inc=1, device_id=target, device_id_type=pl.DeviceIdType.MESH)
    pl.semaphore_wait(barrier, len(targets))


def remote(source, target, send_sem, recv_sem, device_id):
    return pltpu.make_async_remote_copy(
        src_ref=source,
        dst_ref=target,
        send_sem=send_sem,
        recv_sem=recv_sem,
        device_id=device_id,
        device_id_type=pl.DeviceIdType.MESH,
    )


def gather_kernel(count, *refs):
    own_refs, out_refs = refs[:count], refs[count : 2 * count]
    send_sem, recv_sem, local_sem = refs[2 * count :]
    x, near, core = neighbours()
    greet((x, near, core))
    every = []
    for i, (own, out) in enumerate(zip(own_refs, out_refs)):
        n = own.shape[0]
        h = n // 2
        top, bottom = pl.ds(0, h), pl.ds(h, h)

        def copy(number, source, start, rows, to, i=i, out=out):
            return remote(
                source, out.at[pl.ds(start, rows)], send_sem.at[i, number], recv_sem.at[i, number], to
            )

        def again(number, source, start, rows, to, out=out, copy=copy):
            return copy(number, out.at[pl.ds(source, rows)], start, rows, to)

        every.append(
            [
                copy(0, own.at[bottom], n + h, h, x),
                copy(1, own.at[top], 2 * n, h, near),
                copy(2, own.at[top], n, h, x),
                copy(3, own.at[bottom], 2 * n + h, h, near),
                copy(4, own, 4 * n, n, core),
                again(5, 2 * n, 3 * n, h, x),
                again(6, n + h, 3 * n + h, h, near),
                again(7, n, 5 * n, n, core),
                again(8, 2 * n, 6 * n, n, core),
                again(9, 3 * n, 7 * n, n, core),
            ]
        )
    kept = [
        pltpu.make_async_copy(own, out.at[pl.ds(0, own.shape[0])], local_sem.at[i])
        for i, (own, out) in enumerate(zip(own_refs, out_refs))
    ]
    for number in range(5):
        for copies in every:
            copies[number].start()
    for copy in kept:
        copy.start()
    for needs, number in (((1,), 5), ((0,), 6), ((2,), 7), ((3,), 8), ((5, 6), 9)):
        for copies in every:
            for need in needs:
                copies[need].wait_recv()
            copies[number].start()
    for copies in every:
        for number in (4, 7, 8, 9):
            copies[number].wait_recv()
        for copy in copies:
            copy.wait_send()
    for copy in kept:
        copy.wait()


def scatter_kernel(count, *refs):
    part_refs, out_refs = refs[:count], refs[count : 2 * count]
    scratch = refs[2 * count :]
    here_refs, other_refs = scratch[:count], scratch[count : 2 * count]
    stage_refs, land_refs = scratch[2 * count : 3 * count], scratch[3 * count : 4 * count]
    send_sem, recv_sem, local_sem = scratch[4 * count :]
    x, near, core = neighbours()
    greet((x, near, core))
    every, kept = [], []
    for i, part in enumerate(part_refs):
        n = part.shape[0] // 8
        h = n // 2
        copies = {}
        for r in range(4):
            copies[r] = remote(
                part.at[pl.ds((4 + r) * n, n)],
                other_refs[i].at[pl.ds(r * n, n)],
                send_sem.at[i, r],
                recv_sem.at[i, r],
                core,
            )
        for number, start, to in (
            (4, 0, x),
            (5, h, near),
            (6, n, x),
            (7, n + h, x),
            (8, 2 * n, near),
            (9, 2 * n + h, near),
        ):
            copies[number] = remote(
                stage_refs[i].at[pl.ds(start, h)],
                land_refs[i].at[pl.ds(start, h)],
                send_sem.at[i, number],
                recv_sem.at[i, number],
                to,
            )
        every.append(copies)
        kept.append(
            [
                pltpu.make_async_copy(
                    part.at[pl.ds(r * n, n)], here_refs[i].at[pl.ds(r * n, n)], local_sem.at[i, r]
                )
                for r in range(4)
            ]
        )
    order = (3, 1, 2, 0)
    for r in order:
        for i in range(count):
            every[i][r].start()
            kept[i][r].start()

    def add(i, target, start, sources, rows):
        if rows % 16:
            total = sources[0][0][pl.ds(sources[0][1], rows)].astype(F32)
            for ref, first in sources[1:]:
                total = total + ref[pl.ds(first, rows)].astype(F32)
            target[pl.ds(start, rows)] = total.astype(target.dtype)
            return

        def piece(k, carry):
            total = None
            for ref, first in sources:
                value = ref[pl.ds(pl.multiple_of(first + k * 16, 16), 16)].astype(F32)
                total = value if total is None else total + value
            target[pl.ds(pl.multiple_of(start + k * 16, 16), 16)] = total.astype(target.dtype)
            return carry

        lax.fori_loop(0, rows // 16, piece, 0)

    def arrive(r):
        for i in range(count):
            kept[i][r].wait()
            every[i][r].wait_recv()

    sizes = [part.shape[0] // 8 for part in part_refs]
    arrive(3)
    for i, n in enumerate(sizes):
        add(i, stage_refs[i], 0, [(here_refs[i], 3 * n), (other_refs[i], 3 * n)], n)
        every[i][4].start()
        every[i][5].start()
    arrive(1)
    for i, n in enumerate(sizes):
        add(i, stage_refs[i], n, [(here_refs[i], n), (other_refs[i], n)], n // 2)
        every[i][6].start()
    arrive(2)
    for i, n in enumerate(sizes):
        h = n // 2
        add(i, stage_refs[i], 2 * n + h, [(here_refs[i], 2 * n + h), (other_refs[i], 2 * n + h)], h)
        every[i][9].start()
    for i, n in enumerate(sizes):
        h = n // 2
        every[i][5].wait_recv()
        add(
            i,
            stage_refs[i],
            n + h,
            [(here_refs[i], n + h), (other_refs[i], n + h), (land_refs[i], h)],
            h,
        )
        every[i][7].start()
        every[i][4].wait_recv()
        add(i, stage_refs[i], 2 * n, [(here_refs[i], 2 * n), (other_refs[i], 2 * n), (land_refs[i], 0)], h)
        every[i][8].start()
    arrive(0)
    for i, n in enumerate(sizes):
        h = n // 2
        for start, numbers in ((0, (6, 8)), (h, (7, 9))):
            for number in numbers:
                every[i][number].wait_recv()
            add(
                i,
                out_refs[i],
                start,
                [
                    (here_refs[i], start),
                    (other_refs[i], start),
                    (land_refs[i], n + start),
                    (land_refs[i], 2 * n + start),
                ],
                h,
            )
    for copies in every:
        for copy in copies.values():
            copy.wait_send()


IDS = {}


def call_id(kind, arrays):
    key = (kind,) + tuple((item.shape, str(item.dtype)) for item in arrays)
    return IDS.setdefault(key, len(IDS))


def moved_bytes(arrays, factor):
    return sum(item.size * item.dtype.itemsize for item in arrays) * factor


def gather_call(arrays):
    count = len(arrays)

    def body(*refs):
        gather_kernel(count, *refs)

    return pl.pallas_call(
        body,
        name="gather_blocks",
        in_specs=[pl.BlockSpec(memory_space=pltpu.VMEM)] * count,
        out_specs=[pl.BlockSpec(memory_space=pl.ANY)] * count,
        out_shape=[
            jax.ShapeDtypeStruct((8 * item.shape[0],) + item.shape[1:], item.dtype) for item in arrays
        ],
        scratch_shapes=[
            pltpu.SemaphoreType.DMA((count, 10)),
            pltpu.SemaphoreType.DMA((count, 10)),
            pltpu.SemaphoreType.DMA((count,)),
        ],
        compiler_params=pltpu.CompilerParams(
            collective_id=call_id("gather", arrays), has_side_effects=True, vmem_limit_bytes=VMEM_LIMIT
        ),
        cost_estimate=pl.CostEstimate(
            flops=0, bytes_accessed=moved_bytes(arrays, 140), transcendentals=0
        ),
    )(*arrays)


def scatter_call(arrays):
    count = len(arrays)

    def body(*refs):
        scatter_kernel(count, *refs)

    def buffer(item, eighths):
        return pltpu.VMEM((item.shape[0] // 8 * eighths,) + item.shape[1:], item.dtype)

    return pl.pallas_call(
        body,
        name="scatter_blocks",
        in_specs=[pl.BlockSpec(memory_space=pl.ANY)] * count,
        out_specs=[pl.BlockSpec(memory_space=pltpu.VMEM)] * count,
        out_shape=[
            jax.ShapeDtypeStruct((item.shape[0] // 8,) + item.shape[1:], F32) for item in arrays
        ],
        scratch_shapes=[buffer(item, 4) for item in arrays]
        + [buffer(item, 4) for item in arrays]
        + [buffer(item, 3) for item in arrays]
        + [buffer(item, 3) for item in arrays]
        + [
            pltpu.SemaphoreType.DMA((count, 10)),
            pltpu.SemaphoreType.DMA((count, 10)),
            pltpu.SemaphoreType.DMA((count, 4)),
        ],
        compiler_params=pltpu.CompilerParams(
            collective_id=call_id("scatter", arrays), has_side_effects=True, vmem_limit_bytes=VMEM_LIMIT
        ),
        cost_estimate=pl.CostEstimate(
            flops=0, bytes_accessed=moved_bytes(arrays, 18), transcendentals=0
        ),
    )(*arrays)


def place_kernel(flags_ref, total_ref, other_ref, near_total_ref, near_other_ref, *refs):
    out_ref = refs[-1]
    home, first = flags_ref[0] == 1, flags_ref[1] == 1
    rows = total_ref.shape[0]
    for tile in range(total_ref.shape[1] // 128):
        lanes = slice(tile * 128, tile * 128 + 128)
        mine = jnp.where(home, total_ref[:, lanes], near_total_ref[:, lanes]).astype(F32)
        yours = jnp.where(home, other_ref[:, lanes], near_other_ref[:, lanes]).astype(F32)
        stride = 2 * (total_ref.shape[1] // 128)
        out_ref[0, pl.ds(2 * tile, rows, stride=stride), :] = jnp.where(first, mine, yours)
        out_ref[0, pl.ds(2 * tile + 1, rows, stride=stride), :] = jnp.where(first, yours, mine)


def place_inner(depth, flags, parts, target):
    rows, width = parts[0].shape
    step = 256
    per_row = 2 * width // 128
    in_specs = [pl.BlockSpec((step, width), lambda i, flags_ref: (i, 0))] * 4
    operands = list(parts)
    aliases = {}
    if target is not None:
        in_specs = in_specs + [pl.BlockSpec(memory_space=pl.ANY)]
        operands.append(target)
        aliases = {5: 0}
    return pl.pallas_call(
        place_kernel,
        name="place_inner",
        grid_spec=pltpu.PrefetchScalarGridSpec(
            num_scalar_prefetch=1,
            grid=(rows // step,),
            in_specs=in_specs,
            out_specs=pl.BlockSpec((1, step * per_row, 128), lambda i, flags_ref: (depth, i, 0)),
        ),
        out_shape=jax.ShapeDtypeStruct((LAYERS, rows * per_row, 128), F32),
        input_output_aliases=aliases,
        compiler_params=pltpu.CompilerParams(vmem_limit_bytes=VMEM_LIMIT),
        cost_estimate=pl.CostEstimate(flops=0, bytes_accessed=rows * width * 16, transcendentals=0),
    )(flags, *operands)


class Square:
    def __init__(self):
        dp, mp = lax.axis_index("dp"), lax.axis_index("mp")
        core, self.y, far = dp % 2, dp // 2, mp // 4
        self.v = (core * 4 + mp % 4).astype(jnp.int32)
        self.home = core == far

    def swap(self, values):
        return jnp.where(self.home, values, send(values, SWAP))

    def fetch(self, values):
        half = values.shape[0] // 2
        got = send(jnp.where(self.y == 0, values[:half], values[half:]), SWAP)
        other = send(got, AWAY_Y)
        first = jnp.where(self.home, values[:half], jnp.where(self.y == 0, got, other))
        second = jnp.where(self.home, values[half:], jnp.where(self.y == 0, other, got))
        return jnp.concatenate([first, second], axis=0)

    def gather(self, *arrays):
        return gather_call(arrays)

    def scatter(self, *arrays):
        return scatter_call(arrays)

    def scatter_apart(self, part):
        n = part.shape[0] // 8
        half = n // 2
        other = send(part[4 * n :], FLIP_CORE)

        def block(r, at=slice(0, n)):
            rows = slice(r * n + at.start, r * n + at.stop)
            return part[rows].astype(F32) + other[rows].astype(F32)

        top, bottom = slice(0, half), slice(half, n)
        first = send(block(3, top).astype(BF), FLIP_X).astype(F32)
        second = send(block(3, bottom).astype(BF), FLIP_NEAR).astype(F32)
        zeros = jnp.zeros_like(first)
        side = send((block(1) + jnp.concatenate([zeros, second], axis=0)).astype(BF), FLIP_X)
        up = send((block(2) + jnp.concatenate([first, zeros], axis=0)).astype(BF), FLIP_NEAR)
        return block(0) + side.astype(F32) + up.astype(F32)

    def sum_rows(self, values):
        for axis, perm in enumerate((FLIP_CORE, FLIP_NEAR, FLIP_X)):
            values = values + flip_blocks(send(values, perm), axis)
        return values

    def own(self, values):
        return values[: values.shape[0] // 8]

    def reduce_halves(self, first, second):
        mine = jnp.where(self.y == 0, first, second)
        away = jnp.where(self.y == 0, second, first)
        mine = (mine.astype(F32) + send(away, FLIP_Y).astype(F32)).astype(BF)
        total = (mine.astype(F32) + send(mine, TO_HOME).astype(F32)).astype(BF)
        other = send(total, HOME_Y)
        return total, other, send(total, HOME_CORE), send(other, HOME_CORE)

    def reduce_inner(self, depth, part, target):
        width = part.shape[1] // 2
        flags = jnp.stack([self.home, self.y == 0]).astype(jnp.int32)
        parts = self.reduce_halves(part[:, :width], part[:, width:])
        return place_inner(depth, flags, parts, target)

    def inner_result(self, target, results, shape):
        layers, features, two, width = shape
        target = target.reshape(layers, features, width // 128, two, 128)
        return target.transpose(0, 1, 3, 2, 4).reshape(shape)

    def reduce_outer(self, part):
        half = part.shape[0] // 2
        total, other, near_total, near_other = self.reduce_halves(part[:half], part[half:])
        mine = jnp.where(self.home, total, near_total)
        yours = jnp.where(self.home, other, near_other)
        first = jnp.where(self.y == 0, mine, yours)
        second = jnp.where(self.y == 0, yours, mine)
        return jnp.concatenate([first, second], axis=0).astype(F32)

    def reduce_heads(self, part):
        part = part + send(part, FLIP_Y)
        part = part + send(part, TO_HOME)
        return jnp.where(self.home, part, send(part, HOME_CORE))

    def reduce_all(self, part):
        for perm in (FLIP_Y, FLIP_FAR, FLIP_X, FLIP_NEAR, FLIP_CORE):
            part = part + send(part, perm)
        return part

    def split_shared(self, part):
        return xor_blocks(part, self.v)

    def join_shared(self, own):
        own = own + send(own, FLIP_Y)
        own = own + send(own, FLIP_FAR)
        return xor_blocks(self.gather(own.astype(BF))[0], self.v).astype(F32)


class Straight:
    def __init__(self):
        self.v = jnp.int32(0)

    def swap(self, values):
        return values

    fetch = swap

    def gather(self, *arrays):
        return [lax.all_gather(item, "mp", axis=0, tiled=True) for item in arrays]

    def scatter(self, *arrays):
        return [
            lax.psum_scatter(item, "mp", scatter_dimension=0, tiled=True).astype(F32) for item in arrays
        ]

    def scatter_apart(self, part):
        return self.scatter(part)[0]

    def sum_rows(self, values):
        return lax.psum(values, "mp")

    def own(self, values):
        count = values.shape[0] // lax.axis_size("mp")
        return lax.dynamic_slice_in_dim(values, lax.axis_index("mp") * count, count, 0)

    def reduce_inner(self, depth, part, target):
        width = part.shape[1] // 2
        part = lax.psum(part, "dp").astype(F32)
        return jnp.stack([part[:, :width], part[:, width:]], axis=1)

    def inner_result(self, target, results, shape):
        return jnp.stack(results)

    def reduce_outer(self, part):
        return lax.psum(part, "dp").astype(F32)

    def reduce_heads(self, part):
        return lax.psum(part, "dp")

    def reduce_all(self, part):
        return lax.psum(part, AXES)

    def split_shared(self, part):
        return part

    def join_shared(self, own):
        own = lax.psum(own, "dp")
        return lax.all_gather(own, "mp", axis=0, tiled=True)


def local(
    hidden,
    lengths,
    pre_gain,
    w_inner,
    w_step,
    w_shared,
    conv_inner,
    conv_inner_bias,
    conv_shared,
    conv_shared_bias,
    step_bias,
    decay_log,
    skip_gain,
    norm_gain,
    w_out,
    out_grad,
):
    square = lax.axis_size("dp") == 4 and lax.axis_size("mp") == 8 and lengths.shape[0] == 1
    comm = Square() if square else Straight()
    own_rows, features = hidden.shape
    group_rows = lengths.shape[0] * BUCKET
    width = w_inner.shape[3]
    heads = w_step.shape[2]
    total_width = width * lax.axis_size("mp")
    v = comm.v.reshape(1)

    state_low = comm.swap(hidden)
    decay = -jnp.exp(decay_log)
    chan = jnp.concatenate(
        [
            conv_inner,
            conv_inner_bias[:, None],
            norm_gain[:, None],
            jnp.repeat(skip_gain, HEAD_DIM, axis=1)[:, None],
            jnp.zeros((LAYERS, 1, width), F32),
        ],
        axis=1,
    )
    lane_pad = ((0, 0), (0, 0), (0, 128 - heads))
    head = jnp.pad(jnp.stack([step_bias, decay], axis=1), ((0, 0), (0, 6), (0, 128 - heads)))
    chan, head, live = comm.swap(chan), comm.swap(head), comm.swap(lengths)
    steps = jnp.pad(comm.swap(w_step), lane_pad)
    shr = jnp.concatenate(
        [conv_shared, conv_shared_bias[:, None], jnp.zeros((LAYERS, 3, 2 * STATE), F32)], axis=1
    )
    state = state_low.astype(F32)
    last_low = comm.swap(out_grad)
    inner, outer = [], []
    for depth in range(LAYERS):
        fetched = comm.fetch(w_inner[depth].reshape(features, 2 * width))
        inner.append(jnp.concatenate([fetched, w_shared[depth], steps[depth]], axis=1))
        outer.append(comm.fetch(w_out[depth]))

    saved = []
    branches = []
    sums = rates = g_last = None
    for depth in range(LAYERS):
        scale_pre = lax.rsqrt(jnp.mean(state * state, axis=-1, keepdims=True) + EPSILON)
        base = state * scale_pre
        normed = (base * pre_gain[depth]).astype(BF)
        if depth == 0:
            normed, g_last = comm.gather(normed, last_low)
        else:
            (normed,) = comm.gather(normed)
        proj = mm(normed, inner[depth]).astype(BF)
        last = depth == LAYERS - 1
        dsc = mm(g_last, outer[depth], ((1,), (1,))).astype(BF) if last else None
        tall, mixed, states, sums = mixer_forward(
            v, live, own_rows, proj, chan[depth], shr[depth], head[depth], dsc
        )
        part = mm(tall, outer[depth]).astype(BF)
        if last:
            sums = comm.sum_rows(sums[:, 0:2])
            own_sums = comm.own(sums)
            ratio = lax.rsqrt(sums[:, 0] / total_width + EPSILON)
            pull = ratio * ratio * ratio * sums[:, 1] / total_width
            rates = jnp.pad(jnp.stack([ratio, pull], axis=1), ((0, 0), (0, 6), (0, 0)))
            own_part = comm.scatter_apart(part)
        else:
            own_part, own_sums = comm.scatter(part, sums)
        own_ratio = lax.rsqrt(own_sums[:, 0] / total_width + EPSILON)
        branch = own_ratio.reshape(own_rows, 1) * own_part
        branches.append(branch)
        state = state + branch
        saved.append((base, scale_pre, normed, proj, mixed, states, own_ratio, dsc))

    carried = last_low.astype(F32)
    change = 0.0
    target = None
    wide, heads_part, all_part, shared = ([None] * LAYERS for _ in range(4))
    for depth in reversed(range(LAYERS)):
        base, scale_pre, normed, proj, mixed, states, own_ratio, dsc = saved[depth]
        g_full = g_last
        if depth < LAYERS - 1:
            g_low = carried.astype(BF)
            cross = jnp.sum(g_low.astype(F32) * branches[depth], axis=1)
            pull = own_ratio * own_ratio * cross.reshape(own_ratio.shape) / total_width
            rates = jnp.pad(jnp.stack([own_ratio, pull], axis=1), ((0, 0), (0, 6), (0, 0)))
            g_full, rates = comm.gather(g_low, rates)
            dsc = mm(g_full, outer[depth], ((1,), (1,))).astype(BF)
        low, scaled, g_chan, g_shr, g_head = mixer_backward(
            v, live, own_rows, proj, mixed, dsc, states, rates, chan[depth], shr[depth], head[depth]
        )
        part = mm(low, inner[depth], ((1,), (1,))).astype(BF)
        g_small = mm(normed, low[:, 2 * width :], ((0,), (0,)))
        d_normed, shared[depth] = comm.scatter(
            part, comm.split_shared(g_small[:, : 2 * STATE].astype(BF))
        )
        g_inner = mm(normed, low[:, : 2 * width], ((0,), (0,))).astype(BF)
        g_outer = comm.reduce_outer(mm(scaled, g_full, ((0,), (0,))).astype(BF))
        target = comm.reduce_inner(depth, g_inner, target)
        g_step = g_small[:, 2 * STATE : 2 * STATE + heads].T
        wide[depth] = (target, g_outer)
        g_pre = jnp.sum(d_normed * base, axis=0)
        d_base = d_normed * pre_gain[depth]
        moved = scale_pre * (d_base - base * jnp.mean(d_base * base, axis=-1, keepdims=True))
        carried = carried + moved
        change = change + moved
        heads_part[depth] = jnp.concatenate(
            [g_step.reshape(-1, 128), g_chan.reshape(-1, 128), g_head], axis=0
        )
        all_part[depth] = jnp.concatenate([g_pre.reshape(-1, 128), g_shr.reshape(-1, 128)], axis=0)

    first_out = hidden.astype(F32) + comm.swap(branches[0].astype(BF)).astype(F32)
    second_out = first_out + comm.swap(branches[1].astype(BF)).astype(F32)
    hidden_grad = out_grad.astype(F32) + comm.swap(change.astype(BF)).astype(F32)
    joined = comm.join_shared(jnp.concatenate(shared, axis=1))
    per_head = comm.reduce_heads(jnp.stack(heads_part))
    everywhere = comm.reduce_all(jnp.stack(all_part))
    step_rows, chan_rows = heads * features // 128, 8 * width // 128
    g_step = per_head[:, :step_rows].reshape(LAYERS, heads, features).transpose(0, 2, 1)
    g_chan = per_head[:, step_rows : step_rows + chan_rows].reshape(LAYERS, 8, width)
    g_head = per_head[:, step_rows + chan_rows :]
    pre_rows = features // 128
    g_pre = everywhere[:, :pre_rows].reshape(LAYERS, features)
    g_shr = everywhere[:, pre_rows:].reshape(LAYERS, 8, 2 * STATE)
    return (
        first_out,
        second_out,
        hidden_grad,
        g_pre,
        comm.inner_result(target, [item[0] for item in wide], w_inner.shape),
        g_step,
        jnp.stack(jnp.split(joined, LAYERS, axis=1)),
        g_chan[:, 0:4],
        g_chan[:, 4],
        g_shr[:, 0:4],
        g_shr[:, 4],
        g_head[:, 0, :heads],
        g_head[:, 1, :heads] * decay,
        g_chan[:, 6].reshape(LAYERS, heads, HEAD_DIM).sum(axis=-1),
        g_chan[:, 5],
        jnp.stack([item[1] for item in wide]),
    )


def solution(mesh):
    placed = (
        P(("dp", "mp"), None),
        P("dp"),
        P(),
        P(None, None, None, "mp"),
        P(None, None, "mp"),
        P(),
        P(None, None, "mp"),
        P(None, "mp"),
        P(),
        P(),
        P(None, "mp"),
        P(None, "mp"),
        P(None, "mp"),
        P(None, "mp"),
        P(None, "mp", None),
        P(("dp", "mp"), None),
    )
    return jax.shard_map(
        local,
        mesh=mesh,
        in_specs=placed,
        out_specs=(
            P(("dp", "mp"), None),
            P(("dp", "mp"), None),
            P(("dp", "mp"), None),
            P(),
            P(None, None, None, "mp"),
            P(None, None, "mp"),
            P(),
            P(None, None, "mp"),
            P(None, "mp"),
            P(),
            P(),
            P(None, "mp"),
            P(None, "mp"),
            P(None, "mp"),
            P(None, "mp"),
            P(None, "mp", None),
        ),
        check_vma=False,
    )
```
